128 devices in a mesh: blk: 8 (over z, y_hi), rows: 16 (over x, y_lo, core).
Axes of the slice: x: 4, y: 4 (y_hi: 2, y_lo: 2; y = y_hi * 2 + y_lo), z: 4, core: 2. Of those that a mesh axis runs over, the one named last changes fastest.
Arguments:
- embeddings: bfloat16 [65536, 768], P(('blk', 'rows')), as said below
- centroids: bfloat16 [8192, 768], P('blk'), as said below
- log_mix: float32 [8192], P('blk'), may hold values from -1.5 to 3.7
Outputs:
- new_centroids: float32 [8192, 768], P('blk')
- new_weights: float32 [8192], P('blk')
The draws below stay inside these ranges and needn't reach their ends.
Inputs may be any that keep to these rules, and one draw needn't show every extreme that they name: `embeddings`: real vectors of no fixed length. `centroids`: real vectors of no fixed length.
All inputs are finite; a program needn't handle non-finite values.
Results may differ from the reference program's by a relative error of at most 0.0024.
Values may be sent and summed in bfloat16 or wider, within the bound.
A program may use at most 64 MiB of HBM per device.

```python
import math
import jax
import jax.numpy as jnp
from jax import lax

D = 768
K = 8192
NROWS = 65536


def anchor_table(key):
    return jax.random.normal(jax.random.fold_in(key, 101), (K, D), jnp.float32)


def draw_centroids(key, part):
    anchors = anchor_table(key)
    noise_key = jax.random.fold_in(key, 102)
    noise = 0.5 * jax.random.normal(noise_key, (K, D), jnp.float32)
    return (anchors + noise).astype(jnp.bfloat16)


def draw_embeddings(key, part):
    anchors = anchor_table(key)
    assigned = jax.random.randint(jax.random.fold_in(key, 103), (NROWS,), 0, K)
    chosen = anchors[assigned]
    noise_key = jax.random.fold_in(key, 104)
    spread = jnp.exp(jax.random.uniform(jax.random.fold_in(key, 108), (NROWS, 1), jnp.float32, math.log(1.2), math.log(4.0)))
    noise = spread * jax.random.normal(noise_key, (NROWS, D), jnp.float32)
    scales = jnp.exp(jax.random.uniform(jax.random.fold_in(key, 105), (NROWS, 1), jnp.float32, 0.0, math.log(10.0)))
    return ((chosen + noise) * scales).astype(jnp.bfloat16)


def draw_log_mix(key, part):
    position = jnp.arange(K, dtype=jnp.float32) / K
    jitter = jax.random.uniform(jax.random.fold_in(key, 106), (K,), jnp.float32, -1.0, 1.0)
    rising = math.log(9.0) * position
    return jitter + rising


def setup_inputs(seed: int = 0) -> dict:
    key_of = jax.random.split(jax.random.key(seed), 4)
    return {
        "embeddings": draw_embeddings(jax.random.fold_in(key_of[3], 71), 0),
        "centroids": draw_centroids(jax.random.fold_in(key_of[3], 71), 0),
        "log_mix": draw_log_mix(jax.random.fold_in(key_of[3], 71), 0),
    }


concentration = 32.0

def to_unit(values):
    values = values.astype(jnp.float32)
    return (values * lax.rsqrt(lax.optimization_barrier(jnp.sum(values * values, axis=-1, keepdims=True)) + 1e-06)).astype(jnp.bfloat16)

def reference(embeddings, centroids, log_mix):
    centroid_units = to_unit(centroids)
    block_rows = math.gcd(NROWS, 1024)
    grouped = embeddings.reshape(NROWS // block_rows, block_rows, D)

    def accumulate(carried, row_block):
        row_units = to_unit(row_block)
        cosines = jnp.dot(row_units, centroid_units.T, preferred_element_type=jnp.float32)
        scores = jnp.exp(log_mix[None, :] + concentration * (cosines - 1.0))
        totals = lax.optimization_barrier(jnp.sum(scores, axis=1, keepdims=True))
        resp = (scores / totals).astype(jnp.bfloat16)
        weighted = carried[0] + jnp.dot(resp.T, row_units, preferred_element_type=jnp.float32)
        masses = carried[1] + lax.optimization_barrier(jnp.sum(resp.astype(jnp.float32), axis=0))
        return ((weighted, masses), None)
    start_state = (jnp.zeros((K, D), jnp.float32), jnp.zeros((K,), jnp.float32))
    (weighted, masses), _ = lax.scan(accumulate, start_state, grouped)
    new_centroids = weighted * lax.rsqrt(lax.optimization_barrier(jnp.sum(weighted * weighted, axis=1, keepdims=True)) + 1e-06)
    new_weights = masses * (K / NROWS)
    return (new_centroids, new_weights)
```

```python
import math

import jax
import jax.numpy as jnp
from jax import lax
from jax.experimental import pallas as pl
from jax.experimental.pallas import tpu as pltpu
from jax.sharding import PartitionSpec as P

D = 768
CONCENTRATION = 32.0
LOG2E = 1.4426950408889634
MESH = pl.DeviceIdType.MESH
NT = (((1,), (1,)), ((), ()))
NN = (((1,), (0,)), ((), ()))

ROWS = 512
GROUPS = 4
PIECE = 64


def unit(v):
    v = v.astype(jnp.float32)
    return (v * lax.rsqrt(jnp.sum(v * v, axis=1, keepdims=True) + 1e-6)).astype(jnp.bfloat16)


def kernel(
    factor,
    emb, cen, lm, out, wout,
    xr, cr, xu, cu, lmh, lmc, sc, tr, ps, pb, ma, ra, rc, rs, fh, fr, ob, ms, mr, wo,
    in_sem, a_send, a_recv, d_send, d_recv, b_send, b_recv, t_send, t_recv,
    c_send, c_recv, r_send, r_recv, f_send, f_recv, m_send, m_recv, o_send, o_recv,
    q_send, q_recv, w_send, w_recv, out_sem,
):
    blk, row = lax.axis_index("blk"), lax.axis_index("rows")
    z, hi = blk // 2, blk % 2
    x, lo, c = row // 4, (row // 2) % 2, row % 2
    zp, zm, z2 = (z + 1) % 4, (z + 3) % 4, (z + 2) % 4
    xp, xm, x2 = (x + 1) % 4, (x + 3) % 4, (x + 2) % 4
    me8 = z * 2 + c

    def dev(z=z, hi=hi, x=x, lo=lo, c=c):
        return (z * 2 + hi, x * 4 + lo * 2 + c)

    def remote(src, dst, send, recv, to):
        return pltpu.make_async_remote_copy(
            src_ref=src, dst_ref=dst, send_sem=send, recv_sem=recv, device_id=to, device_id_type=MESH
        )

    started = []

    def go(src, dst, send, recv, to):
        copy = remote(src, dst, send, recv, to)
        copy.start()
        started.append(copy)

    def landed(dst, send, recv):
        remote(dst, dst, send, recv, dev(c=1 - c)).wait_recv()

    get_x = pltpu.make_async_copy(emb, xr, in_sem.at[0])
    get_c = pltpu.make_async_copy(cen.at[pl.ds(pl.multiple_of(c * 512, 512), 512)], cr, in_sem.at[1])
    get_x.start()
    get_c.start()

    line = [dev(c=1 - c)] + [dev(z=zz, c=cc) for zz in (zp, zm, z2) for cc in (0, 1)]
    near = [dev(lo=1 - lo)] + [dev(x=xx, lo=ll) for xx in (xp, xm, x2) for ll in (0, 1)]
    across = [dev(hi=1 - hi, x=xx, lo=ll) for xx in range(4) for ll in (0, 1)]
    barrier = pltpu.get_barrier_semaphore()
    for peer in line + near + across:
        pl.semaphore_signal(barrier, inc=1, device_id=peer, device_id_type=MESH)

    get_x.wait()

    def unit_rows(i, _):
        v = unit(xr[pl.ds(pl.multiple_of(i * 64, 64), 64)])
        xu[i // 2, z, c, pl.ds(pl.multiple_of(i % 2 * 64, 64), 64)] = v
        return 0

    lax.fori_loop(0, ROWS // 64, unit_rows, 0)
    get_c.wait()

    def unit_centroids(i, _):
        cu[i] = unit(cr[pl.ds(pl.multiple_of(i * 64, 64), 64)])
        return 0

    lax.fori_loop(0, 8, unit_centroids, 0)

    def offsets(i, ref, turn, base):
        r = ref[pl.ds(c * 4 + i, 1), :]
        wide = jnp.broadcast_to(r, (128, 128))
        if turn:
            wide = pltpu.roll(wide, 64, 1)
        lmc[base + i] = (wide.T - CONCENTRATION) * LOG2E

    for i in range(4):
        offsets(i, lm, False, 0)

    def clear(i, _):
        ps[i] = jnp.zeros((PIECE, D), jnp.float32)
        return 0

    lax.fori_loop(0, 16, clear, 0)
    ma[...] = jnp.zeros_like(ma)
    pl.semaphore_wait(barrier, len(line + near + across))

    def piece(g, zs, e):
        return xu.at[g, zs, c, pl.ds(e * 64, 64)]

    def rows_out(g):
        for e in (0, 1):
            at = piece(g, z, e)
            go(at, at, a_send.at[g, e], a_recv.at[g, e], dev(z=zp))
            go(at, at, a_send.at[g, 2 + e], a_recv.at[g, 2 + e], dev(z=zm))

    def share(g, zs, k):
        at = xu.at[g, zs, c]
        go(at, at, d_send.at[g, k], d_recv.at[g, k], dev(c=1 - c))

    def rows_came(g, zs, e, k):
        landed(piece(g, zs, e), a_send.at[g, k], a_recv.at[g, k])

    def neighbours_in(g):
        rows_came(g, zm, 0, 0)
        at = piece(g, zm, 0)
        go(at, at, a_send.at[g, 4], a_recv.at[g, 4], dev(z=zp))
        rows_came(g, zp, 1, 3)
        at = piece(g, zp, 1)
        go(at, at, a_send.at[g, 5], a_recv.at[g, 5], dev(z=zm))
        if g + 2 < GROUPS:
            rows_out(g + 2)
        rows_came(g, zm, 1, 1)
        share(g, zm, 1)
        rows_came(g, zp, 0, 2)
        share(g, zp, 2)

    def far_in(g):
        rows_came(g, z2, 0, 4)
        rows_came(g, z2, 1, 5)
        share(g, z2, 3)

    def shared(g):
        for zs, k in ((z, 0), (zm, 1), (zp, 2), (z2, 3)):
            landed(xu.at[g, zs, 1 - c], d_send.at[g, k], d_recv.at[g, k])

    rows_out(0)
    rows_out(1)
    for g in range(GROUPS):
        share(g, z, 0)
    opposite = dev(hi=1 - hi, lo=1 - lo)
    for i in range(8):
        copy = remote(cu.at[i], cu.at[8 + (i ^ 1)], b_send.at[0], b_recv.at[0], opposite)
        copy.start()
    go(lm, lmh, b_send.at[1], b_recv.at[1], opposite)

    def block(g, n):
        return xu[g, pl.ds(n * 2, 2)].reshape(512, D)

    def scores(g, h):
        def zero(n, _):
            tr[g, me8, n] = jnp.zeros((1, 512), jnp.float32)
            return 0

        def add(m, _):
            n, i = m // 2, m % 2
            cos = lax.dot_general(
                cu[pl.ds(h * 8 + i * 4, 4)].reshape(256, D), block(g, n), NT,
                preferred_element_type=jnp.float32,
            )
            off = lmc[pl.ds(h * 4 + i * 2, 2)].reshape(256, 128)
            off = jnp.concatenate([off] * 4, axis=1)
            e = jnp.exp2(cos * (CONCENTRATION * LOG2E) + off)
            sc[g, n, pl.ds(pl.multiple_of(h * 512 + i * 256, 256), 256)] = e
            tr[g, me8, n] = tr[g, me8, n] + jnp.sum(e, axis=0, keepdims=True)
            return 0

        if h == 0:
            lax.fori_loop(0, 2, zero, 0)
        lax.fori_loop(0, 4, add, 0)

    def totals_out(zs):
        for peer in line:
            remote(tr.at[zs, me8], tr.at[zs, me8], t_send.at[zs], t_recv.at[zs], peer).start()

    def totals_in(zs):
        all7 = tr.at[zs, pl.ds(0, 7)]
        landed(all7, t_send.at[zs], t_recv.at[zs])

    def inverse(zs):
        return 1.0 / jnp.sum(tr[zs], axis=0)

    def weigh(zs, begin, end):
        inv = inverse(zs)

        def body(i, _):
            acc = ps[pl.ds(i * 4, 4)].reshape(256, D)
            mass = ma[pl.ds(i * 2, 2)].reshape(256, 128)
            for plane in range(2):
                r = sc[zs, plane, pl.ds(pl.multiple_of(i * 256, 256), 256)] * inv[plane]
                for q in range(4):
                    mass = mass + r[:, q * 128 : (q + 1) * 128]
                acc = acc + lax.dot_general(
                    r.astype(jnp.bfloat16), block(zs, plane), NN, preferred_element_type=jnp.float32
                )
            ps[pl.ds(i * 4, 4)] = acc.reshape(4, PIECE, D)
            ma[pl.ds(i * 2, 2)] = mass.reshape(2, 128, 128)
            return 0

        lax.fori_loop(begin, end, body, 0)

    neighbours_in(0)
    neighbours_in(1)
    far_in(0)
    shared(0)
    scores(0, 0)
    neighbours_in(2)
    far_in(1)
    shared(1)
    scores(1, 0)
    landed(cu.at[pl.ds(8, 8)], b_send.at[0], b_recv.at[0])
    landed(lmh, b_send.at[1], b_recv.at[1])
    for i in range(4):
        offsets(i, lmh, True, 4)
    scores(0, 1)
    totals_out(0)
    scores(1, 1)
    totals_out(1)
    neighbours_in(3)
    far_in(2)
    totals_in(0)
    weigh(0, 0, 4)
    shared(2)
    scores(2, 0)
    scores(2, 1)
    totals_out(2)
    totals_in(1)
    weigh(1, 0, 4)
    far_in(3)
    shared(3)
    scores(3, 0)
    scores(3, 1)
    totals_out(3)
    totals_in(2)
    weigh(2, 0, 4)
    totals_in(3)

    def pack(ch):
        def body(i, _):
            pb[i] = ps[i].astype(jnp.bfloat16)
            return 0

        lax.fori_loop(ch * 8, ch * 8 + 8, body, 0)

    def scatter(ch):
        base = ch * 8

        def send(k, src, slot, to):
            go(src, rc.at[ch, slot], c_send.at[ch, k], c_recv.at[ch, slot], to)

        go(pb.at[base + x2 * 2], ra.at[ch, 0], r_send.at[ch, 0], r_recv.at[ch, 0], dev(x=xp))
        go(pb.at[base + x2 * 2 + 1], ra.at[ch, 1], r_send.at[ch, 1], r_recv.at[ch, 1], dev(x=xm))
        send(0, pb.at[base + xp * 2 + 1], lo, dev(x=xp, lo=1))
        send(1, pb.at[base + xm * 2], 2 + lo, dev(x=xm, lo=0))
        send(2, pb.at[base + x * 2 + 1 - lo], 4, dev(lo=1 - lo))

    def relay(ch):
        base = ch * 8
        landed(ra.at[ch, 0], r_send.at[ch, 0], r_recv.at[ch, 0])
        rs[ch, 0] = (ps[base + xp * 2] + ra[ch, 0].astype(jnp.float32)).astype(jnp.bfloat16)
        go(rs.at[ch, 0], rc.at[ch, lo], c_send.at[ch, 3], c_recv.at[ch, lo], dev(x=xp, lo=0))
        landed(ra.at[ch, 1], r_send.at[ch, 1], r_recv.at[ch, 1])
        rs[ch, 1] = (ps[base + xm * 2 + 1] + ra[ch, 1].astype(jnp.float32)).astype(jnp.bfloat16)
        go(rs.at[ch, 1], rc.at[ch, 2 + lo], c_send.at[ch, 4], c_recv.at[ch, 2 + lo], dev(x=xm, lo=1))

    def gathered(ch):
        total = ps[ch * 8 + x * 2 + lo]
        for slot in (4, 0, 1, 2, 3):
            landed(rc.at[ch, slot], c_send.at[ch, 0], c_recv.at[ch, slot])
            total = total + rc[ch, slot].astype(jnp.float32)
        return total

    weigh(3, 2, 4)
    pack(1)
    scatter(1)
    weigh(3, 0, 2)
    pack(0)
    scatter(0)

    for i in range(8):
        r = jnp.sum(ma[i].T, axis=0, keepdims=True)
        if i >= 4:
            r = pltpu.roll(jnp.broadcast_to(r, (8, 128)), 64, 1)[0:1]
        ms[i // 4, pl.ds(i % 4, 1)] = r
    mine = x * 2 + lo
    for peer in near:
        remote(ms.at[0], mr.at[mine], m_send, m_recv, peer).start()
    for peer in across:
        remote(ms.at[1], mr.at[8 + mine], m_send, m_recv, peer).start()
    mr[mine] = ms[0]

    relay(1)
    relay(0)
    fh[...] = gathered(1).astype(jnp.bfloat16)
    go(fh, fr, f_send.at[0], f_recv.at[0], opposite)
    total = gathered(0)
    landed(fr, f_send.at[0], f_recv.at[0])
    total = total + fr[...].astype(jnp.float32)
    done = total * lax.rsqrt(jnp.sum(total * total, axis=1, keepdims=True) + 1e-6)
    ob[c, x, lo] = done.astype(jnp.bfloat16)

    def hand(xx, ll, k, recv, to):
        at = ob.at[c, xx, ll]
        go(at, at, o_send.at[k], o_recv.at[recv], to)

    def handed(xx, ll, recv):
        landed(ob.at[c, xx, ll], o_send.at[0], o_recv.at[recv])

    def twin(xx, ll, k):
        at = ob.at[c, xx, ll]
        go(at, at, q_send.at[k], q_recv.at[k], dev(c=1 - c))

    for ll in (0, 1):
        hand(x, lo, ll, 1 + lo, dev(x=xp, lo=ll))
        hand(x, lo, 2 + ll, 3 + lo, dev(x=xm, lo=ll))
    hand(x, lo, 4, 0, dev(lo=1 - lo))
    twin(x, lo, 0)

    landed(mr.at[pl.ds(0, 15)], m_send, m_recv)
    wo[c] = jnp.sum(mr[...], axis=0) * factor
    go(wo.at[c], wo.at[c], w_send.at[0], w_recv.at[0], dev(c=1 - c))

    handed(xm, 0, 1)
    hand(xm, 0, 5, 5, dev(x=xp))
    handed(xp, 1, 4)
    hand(xp, 1, 6, 6, dev(x=xm))
    twin(xm, 0, 1)
    twin(xp, 1, 2)
    handed(xm, 1, 2)
    twin(xm, 1, 3)
    handed(xp, 0, 3)
    twin(xp, 0, 4)
    handed(x, 1 - lo, 0)
    twin(x, 1 - lo, 5)
    handed(x2, 0, 5)
    twin(x2, 0, 6)
    handed(x2, 1, 6)
    twin(x2, 1, 7)
    for k, (xx, ll) in enumerate(
        ((x, lo), (xm, 0), (xp, 1), (xm, 1), (xp, 0), (x, 1 - lo), (x2, 0), (x2, 1))
    ):
        landed(ob.at[1 - c, xx, ll], q_send.at[k], q_recv.at[k])
    landed(wo.at[1 - c], w_send.at[0], w_recv.at[0])
    put = pltpu.make_async_copy(ob, out, out_sem.at[0])
    put.start()
    put_w = pltpu.make_async_copy(wo, wout, out_sem.at[1])
    put_w.start()

    for copy in started:
        copy.wait_send()
    everything = dev(c=1 - c)
    remote(cu.at[pl.ds(8, 8)], cu.at[pl.ds(8, 8)], b_send.at[0], b_recv.at[0], everything).wait_send()
    for zs in range(4):
        all7 = tr.at[zs, pl.ds(0, 7)]
        remote(all7, all7, t_send.at[zs], t_recv.at[zs], everything).wait_send()
    m15 = mr.at[pl.ds(0, 15)]
    remote(m15, m15, m_send, m_recv, everything).wait_send()
    put.wait()
    put_w.wait()


def local(embeddings, centroids, log_mix, factor):
    f32, bf16 = jnp.float32, jnp.bfloat16
    dma = pltpu.SemaphoreType.DMA
    vmem = pltpu.VMEM
    any_spec = pl.BlockSpec(memory_space=pl.ANY)
    body = lambda *refs: kernel(factor, *refs)
    made, weights = pl.pallas_call(
        body,
        out_shape=(
            jax.ShapeDtypeStruct((2, 4, 2, PIECE, D), bf16),
            jax.ShapeDtypeStruct((2, 4, 128), f32),
        ),
        in_specs=[any_spec, any_spec, pl.BlockSpec(memory_space=vmem)],
        out_specs=(any_spec, any_spec),
        scratch_shapes=[
            vmem((ROWS, D), bf16),
            vmem((512, D), bf16),
            vmem((GROUPS, 4, 2, 128, D), bf16),
            vmem((16, PIECE, D), bf16),
            vmem((8, 128), f32),
            vmem((8, 128, 128), f32),
            vmem((4, 2, 1024, ROWS), f32),
            vmem((4, 8, 2, 1, ROWS), f32),
            vmem((16, PIECE, D), f32),
            vmem((16, PIECE, D), bf16),
            vmem((8, 128, 128), f32),
            vmem((2, 2, PIECE, D), bf16),
            vmem((2, 5, PIECE, D), bf16),
            vmem((2, 2, PIECE, D), bf16),
            vmem((PIECE, D), bf16),
            vmem((PIECE, D), bf16),
            vmem((2, 4, 2, PIECE, D), bf16),
            vmem((2, 4, 128), f32),
            vmem((16, 4, 128), f32),
            vmem((2, 4, 128), f32),
            dma((2,)),
            dma((GROUPS, 6)), dma((GROUPS, 6)),
            dma((GROUPS, 4)), dma((GROUPS, 4)),
            dma((2,)), dma((2,)),
            dma((4,)), dma((4,)),
            dma((2, 5)), dma((2, 5)),
            dma((2, 2)), dma((2, 2)),
            dma((1,)), dma((1,)),
            dma, dma,
            dma((7,)), dma((7,)),
            dma((8,)), dma((8,)),
            dma((1,)), dma((1,)),
            dma((2,)),
        ],
        compiler_params=pltpu.CompilerParams(
            collective_id=0, has_side_effects=True, vmem_limit_bytes=60 * 1024 * 1024
        ),
        cost_estimate=pl.CostEstimate(flops=13 * 10**9, bytes_accessed=10**7, transcendentals=4 * 10**6),
        name="em_step",
    )(embeddings, centroids, log_mix.reshape(8, 128))
    return made.reshape(1024, D).astype(f32), weights.reshape(1024)


def solution(mesh):
    blks, rows = mesh.shape["blk"], mesh.shape["rows"]

    def step(embeddings, centroids, log_mix):
        factor = centroids.shape[0] * blks / (embeddings.shape[0] * blks * rows)
        return local(embeddings, centroids, log_mix, factor)

    return jax.shard_map(
        step,
        mesh=mesh,
        in_specs=(P(("blk", "rows"), None), P("blk", None), P("blk")),
        out_specs=(P("blk", None), P("blk")),
        check_vma=False,
    )
```

```python
import math

import jax
import jax.numpy as jnp
from jax import lax
from jax.experimental import pallas as pl
from jax.experimental.pallas import tpu as pltpu
from jax.sharding import PartitionSpec as P

D = 768
CONCENTRATION = 32.0
LOG2E = 1.4426950408889634
MESH = pl.DeviceIdType.MESH
NT = (((1,), (1,)), ((), ()))
NN = (((1,), (0,)), ((), ()))

ROWS = 512
GROUPS = 4
PIECE = 64


def unit(v):
    v = v.astype(jnp.float32)
    return (v * lax.rsqrt(jnp.sum(v * v, axis=1, keepdims=True) + 1e-6)).astype(jnp.bfloat16)


def kernel(
    factor,
    emb, cen, lm, out, wout,
    xr, cr, xu, cu, lmh, lmc, sc, tr, ps, pb, ma, ra, rc, rs, fh, fr, ob, ms, mr, wo,
    in_sem, a_send, a_recv, d_send, d_recv, b_send, b_recv, t_send, t_recv,
    c_send, c_recv, r_send, r_recv, f_send, f_recv, m_send, m_recv, o_send, o_recv,
    q_send, q_recv, w_send, w_recv, out_sem,
):
    blk, row = lax.axis_index("blk"), lax.axis_index("rows")
    z, hi = blk // 2, blk % 2
    x, lo, c = row // 4, (row // 2) % 2, row % 2
    zp, zm, z2 = (z + 1) % 4, (z + 3) % 4, (z + 2) % 4
    xp, xm, x2 = (x + 1) % 4, (x + 3) % 4, (x + 2) % 4
    me8 = z * 2 + c

    def dev(z=z, hi=hi, x=x, lo=lo, c=c):
        return (z * 2 + hi, x * 4 + lo * 2 + c)

    def remote(src, dst, send, recv, to):
        return pltpu.make_async_remote_copy(
            src_ref=src, dst_ref=dst, send_sem=send, recv_sem=recv, device_id=to, device_id_type=MESH
        )

    started = []

    def go(src, dst, send, recv, to):
        copy = remote(src, dst, send, recv, to)
        copy.start()
        started.append(copy)

    def landed(dst, send, recv):
        remote(dst, dst, send, recv, dev(c=1 - c)).wait_recv()

    get_x = pltpu.make_async_copy(emb, xr, in_sem.at[0])
    get_c = pltpu.make_async_copy(cen.at[pl.ds(pl.multiple_of(c * 512, 512), 512)], cr, in_sem.at[1])
    get_x.start()
    get_c.start()

    line = [dev(c=1 - c)] + [dev(z=zz, c=cc) for zz in (zp, zm, z2) for cc in (0, 1)]
    near = [dev(lo=1 - lo)] + [dev(x=xx, lo=ll) for xx in (xp, xm, x2) for ll in (0, 1)]
    across = [dev(hi=1 - hi, x=xx, lo=ll) for xx in range(4) for ll in (0, 1)]
    barrier = pltpu.get_barrier_semaphore()
    for peer in line + near + across:
        pl.semaphore_signal(barrier, inc=1, device_id=peer, device_id_type=MESH)

    get_x.wait()

    def unit_rows(i, _):
        v = unit(xr[pl.ds(pl.multiple_of(i * 64, 64), 64)])
        xu[i // 2, z, c, pl.ds(pl.multiple_of(i % 2 * 64, 64), 64)] = v
        return 0

    lax.fori_loop(0, ROWS // 64, unit_rows, 0)
    get_c.wait()

    def unit_centroids(i, _):
        cu[i] = unit(cr[pl.ds(pl.multiple_of(i * 64, 64), 64)])
        return 0

    lax.fori_loop(0, 8, unit_centroids, 0)

    def offsets(i, ref, turn, base):
        r = ref[pl.ds(c * 4 + i, 1), :]
        wide = jnp.broadcast_to(r, (128, 128))
        if turn:
            wide = pltpu.roll(wide, 64, 1)
        lmc[base + i] = (wide.T - CONCENTRATION) * LOG2E

    for i in range(4):
        offsets(i, lm, False, 0)

    def clear(i, _):
        ps[i] = jnp.zeros((PIECE, D), jnp.float32)
        return 0

    lax.fori_loop(0, 16, clear, 0)
    ma[...] = jnp.zeros_like(ma)
    pl.semaphore_wait(barrier, len(line + near + across))

    def piece(g, zs, e):
        return xu.at[g, zs, c, pl.ds(e * 64, 64)]

    def rows_out(g):
        for e in (0, 1):
            at = piece(g, z, e)
            go(at, at, a_send.at[g, e], a_recv.at[g, e], dev(z=zp))
            go(at, at, a_send.at[g, 2 + e], a_recv.at[g, 2 + e], dev(z=zm))

    def share(g, zs, k):
        at = xu.at[g, zs, c]
        go(at, at, d_send.at[g, k], d_recv.at[g, k], dev(c=1 - c))

    def rows_came(g, zs, e, k):
        landed(piece(g, zs, e), a_send.at[g, k], a_recv.at[g, k])

    def neighbours_in(g):
        rows_came(g, zm, 0, 0)
        at = piece(g, zm, 0)
        go(at, at, a_send.at[g, 4], a_recv.at[g, 4], dev(z=zp))
        rows_came(g, zp, 1, 3)
        at = piece(g, zp, 1)
        go(at, at, a_send.at[g, 5], a_recv.at[g, 5], dev(z=zm))
        if g + 2 < GROUPS:
            rows_out(g + 2)
        rows_came(g, zm, 1, 1)
        share(g, zm, 1)
        rows_came(g, zp, 0, 2)
        share(g, zp, 2)

    def far_in(g):
        rows_came(g, z2, 0, 4)
        rows_came(g, z2, 1, 5)
        share(g, z2, 3)

    def shared(g):
        for zs, k in ((z, 0), (zm, 1), (zp, 2), (z2, 3)):
            landed(xu.at[g, zs, 1 - c], d_send.at[g, k], d_recv.at[g, k])

    rows_out(0)
    rows_out(1)
    for g in range(GROUPS):
        share(g, z, 0)
    opposite = dev(hi=1 - hi, lo=1 - lo)
    for i in range(8):
        copy = remote(cu.at[i], cu.at[8 + (i ^ 1)], b_send.at[0], b_recv.at[0], opposite)
        copy.start()
    go(lm, lmh, b_send.at[1], b_recv.at[1], opposite)

    def scores(g, h):
        def add(n, _):
            cos = lax.dot_general(
                cu[pl.ds(h * 8, 8)].reshape(512, D), xu[g, n].reshape(256, D), NT,
                preferred_element_type=jnp.float32,
            )
            off = lmc[pl.ds(h * 4, 4)].reshape(512, 128)
            e = jnp.exp2(cos * (CONCENTRATION * LOG2E) + jnp.concatenate([off] * 2, axis=1))
            sc[g, n, pl.ds(h * 512, 512)] = e
            part = jnp.sum(e, axis=0, keepdims=True)
            tr[g, me8, n] = part if h == 0 else tr[g, me8, n] + part
            return 0

        lax.fori_loop(0, 4, add, 0, unroll=4)

    def totals_out(zs):
        for peer in line:
            remote(tr.at[zs, me8], tr.at[zs, me8], t_send.at[zs], t_recv.at[zs], peer).start()

    def totals_in(zs):
        all7 = tr.at[zs, pl.ds(0, 7)]
        landed(all7, t_send.at[zs], t_recv.at[zs])

    def inverse(zs):
        return 1.0 / jnp.sum(tr[zs], axis=0)

    def weigh(g, begin, end):
        inv = inverse(g)

        def body(i, _):
            acc = ps[pl.ds(i * 4, 4)].reshape(256, D)
            mass = ma[pl.ds(i * 2, 2)].reshape(256, 128)
            resp = []
            for n in range(4):
                r = sc[g, n, pl.ds(pl.multiple_of(i * 256, 256), 256)] * inv[n]
                mass = mass + r[:, :128] + r[:, 128:]
                resp.append(r.astype(jnp.bfloat16))
            acc = acc + lax.dot_general(
                jnp.concatenate(resp, axis=1), xu[g].reshape(1024, D), NN, preferred_element_type=jnp.float32
            )
            ps[pl.ds(i * 4, 4)] = acc.reshape(4, PIECE, D)
            ma[pl.ds(i * 2, 2)] = mass.reshape(2, 128, 128)
            return 0

        lax.fori_loop(begin, end, body, 0, unroll=2)

    neighbours_in(0)
    neighbours_in(1)
    far_in(0)
    shared(0)
    scores(0, 0)
    neighbours_in(2)
    far_in(1)
    shared(1)
    scores(1, 0)
    landed(cu.at[pl.ds(8, 8)], b_send.at[0], b_recv.at[0])
    landed(lmh, b_send.at[1], b_recv.at[1])
    for i in range(4):
        offsets(i, lmh, True, 4)
    scores(0, 1)
    totals_out(0)
    scores(1, 1)
    totals_out(1)
    neighbours_in(3)
    far_in(2)
    totals_in(0)
    weigh(0, 0, 4)
    shared(2)
    scores(2, 0)
    scores(2, 1)
    totals_out(2)
    totals_in(1)
    weigh(1, 0, 4)
    far_in(3)
    shared(3)
    scores(3, 0)
    scores(3, 1)
    totals_out(3)
    totals_in(2)
    weigh(2, 0, 4)
    totals_in(3)

    def pack(ch):
        def body(i, _):
            pb[i] = ps[i].astype(jnp.bfloat16)
            return 0

        lax.fori_loop(ch * 8, ch * 8 + 8, body, 0)

    def scatter(ch):
        base = ch * 8

        def send(k, src, slot, to):
            go(src, rc.at[ch, slot], c_send.at[ch, k], c_recv.at[ch, slot], to)

        go(pb.at[base + x2 * 2], ra.at[ch, 0], r_send.at[ch, 0], r_recv.at[ch, 0], dev(x=xp))
        go(pb.at[base + x2 * 2 + 1], ra.at[ch, 1], r_send.at[ch, 1], r_recv.at[ch, 1], dev(x=xm))
        send(0, pb.at[base + xp * 2 + 1], lo, dev(x=xp, lo=1))
        send(1, pb.at[base + xm * 2], 2 + lo, dev(x=xm, lo=0))
        send(2, pb.at[base + x * 2 + 1 - lo], 4, dev(lo=1 - lo))

    def relay(ch):
        base = ch * 8
        landed(ra.at[ch, 0], r_send.at[ch, 0], r_recv.at[ch, 0])
        rs[ch, 0] = (ps[base + xp * 2] + ra[ch, 0].astype(jnp.float32)).astype(jnp.bfloat16)
        go(rs.at[ch, 0], rc.at[ch, lo], c_send.at[ch, 3], c_recv.at[ch, lo], dev(x=xp, lo=0))
        landed(ra.at[ch, 1], r_send.at[ch, 1], r_recv.at[ch, 1])
        rs[ch, 1] = (ps[base + xm * 2 + 1] + ra[ch, 1].astype(jnp.float32)).astype(jnp.bfloat16)
        go(rs.at[ch, 1], rc.at[ch, 2 + lo], c_send.at[ch, 4], c_recv.at[ch, 2 + lo], dev(x=xm, lo=1))

    def gathered(ch):
        total = ps[ch * 8 + x * 2 + lo]
        for slot in (4, 0, 1, 2, 3):
            landed(rc.at[ch, slot], c_send.at[ch, 0], c_recv.at[ch, slot])
            total = total + rc[ch, slot].astype(jnp.float32)
        return total

    weigh(3, 2, 4)
    pack(1)
    scatter(1)
    weigh(3, 0, 2)
    pack(0)
    scatter(0)

    for i in range(8):
        r = jnp.sum(ma[i].T, axis=0, keepdims=True)
        if i >= 4:
            r = pltpu.roll(jnp.broadcast_to(r, (8, 128)), 64, 1)[0:1]
        ms[i // 4, pl.ds(i % 4, 1)] = r
    mine = x * 2 + lo
    for peer in near:
        remote(ms.at[0], mr.at[mine], m_send, m_recv, peer).start()
    for peer in across:
        remote(ms.at[1], mr.at[8 + mine], m_send, m_recv, peer).start()
    mr[mine] = ms[0]

    relay(1)
    relay(0)
    fh[...] = gathered(1)
    go(fh, fr, f_send.at[0], f_recv.at[0], opposite)
    total = gathered(0)
    landed(fr, f_send.at[0], f_recv.at[0])
    total = total + fr[...]
    done = total * lax.rsqrt(jnp.sum(total * total, axis=1, keepdims=True) + 1e-6)
    ob[c, x, lo] = done.astype(jnp.bfloat16)

    def hand(xx, ll, k, recv, to):
        at = ob.at[c, xx, ll]
        go(at, at, o_send.at[k], o_recv.at[recv], to)

    def handed(xx, ll, recv):
        landed(ob.at[c, xx, ll], o_send.at[0], o_recv.at[recv])

    def twin(xx, ll, k):
        at = ob.at[c, xx, ll]
        go(at, at, q_send.at[k], q_recv.at[k], dev(c=1 - c))

    for ll in (0, 1):
        hand(x, lo, ll, 1 + lo, dev(x=xp, lo=ll))
        hand(x, lo, 2 + ll, 3 + lo, dev(x=xm, lo=ll))
    hand(x, lo, 4, 0, dev(lo=1 - lo))
    twin(x, lo, 0)

    landed(mr.at[pl.ds(0, 15)], m_send, m_recv)
    wo[c] = jnp.sum(mr[...], axis=0) * factor
    go(wo.at[c], wo.at[c], w_send.at[0], w_recv.at[0], dev(c=1 - c))

    handed(xm, 0, 1)
    hand(xm, 0, 5, 5, dev(x=xp))
    handed(xp, 1, 4)
    hand(xp, 1, 6, 6, dev(x=xm))
    twin(xm, 0, 1)
    twin(xp, 1, 2)
    handed(xm, 1, 2)
    twin(xm, 1, 3)
    handed(xp, 0, 3)
    twin(xp, 0, 4)
    handed(x, 1 - lo, 0)
    twin(x, 1 - lo, 5)
    handed(x2, 0, 5)
    twin(x2, 0, 6)
    handed(x2, 1, 6)
    twin(x2, 1, 7)
    for k, (xx, ll) in enumerate(
        ((x, lo), (xm, 0), (xp, 1), (xm, 1), (xp, 0), (x, 1 - lo), (x2, 0), (x2, 1))
    ):
        landed(ob.at[1 - c, xx, ll], q_send.at[k], q_recv.at[k])
    landed(wo.at[1 - c], w_send.at[0], w_recv.at[0])
    put = pltpu.make_async_copy(ob, out, out_sem.at[0])
    put.start()
    put_w = pltpu.make_async_copy(wo, wout, out_sem.at[1])
    put_w.start()

    for copy in started:
        copy.wait_send()
    everything = dev(c=1 - c)
    remote(cu.at[pl.ds(8, 8)], cu.at[pl.ds(8, 8)], b_send.at[0], b_recv.at[0], everything).wait_send()
    for zs in range(4):
        all7 = tr.at[zs, pl.ds(0, 7)]
        remote(all7, all7, t_send.at[zs], t_recv.at[zs], everything).wait_send()
    m15 = mr.at[pl.ds(0, 15)]
    remote(m15, m15, m_send, m_recv, everything).wait_send()
    put.wait()
    put_w.wait()


def local(embeddings, centroids, log_mix, factor):
    f32, bf16 = jnp.float32, jnp.bfloat16
    dma = pltpu.SemaphoreType.DMA
    vmem = pltpu.VMEM
    any_spec = pl.BlockSpec(memory_space=pl.ANY)
    body = lambda *refs: kernel(factor, *refs)
    made, weights = pl.pallas_call(
        body,
        out_shape=(
            jax.ShapeDtypeStruct((2, 4, 2, PIECE, D), bf16),
            jax.ShapeDtypeStruct((2, 4, 128), f32),
        ),
        in_specs=[any_spec, any_spec, pl.BlockSpec(memory_space=vmem)],
        out_specs=(any_spec, any_spec),
        scratch_shapes=[
            vmem((ROWS, D), bf16),
            vmem((512, D), bf16),
            vmem((GROUPS, 4, 2, 128, D), bf16),
            vmem((16, PIECE, D), bf16),
            vmem((8, 128), f32),
            vmem((8, 128, 128), f32),
            vmem((4, 4, 1024, 256), f32),
            vmem((4, 8, 4, 1, 256), f32),
            vmem((16, PIECE, D), f32),
            vmem((16, PIECE, D), bf16),
            vmem((8, 128, 128), f32),
            vmem((2, 2, PIECE, D), bf16),
            vmem((2, 5, PIECE, D), bf16),
            vmem((2, 2, PIECE, D), bf16),
            vmem((PIECE, D), f32),
            vmem((PIECE, D), f32),
            vmem((2, 4, 2, PIECE, D), bf16),
            vmem((2, 4, 128), f32),
            vmem((16, 4, 128), f32),
            vmem((2, 4, 128), f32),
            dma((2,)),
            dma((GROUPS, 6)), dma((GROUPS, 6)),
            dma((GROUPS, 4)), dma((GROUPS, 4)),
            dma((2,)), dma((2,)),
            dma((4,)), dma((4,)),
            dma((2, 5)), dma((2, 5)),
            dma((2, 2)), dma((2, 2)),
            dma((1,)), dma((1,)),
            dma, dma,
            dma((7,)), dma((7,)),
            dma((8,)), dma((8,)),
            dma((1,)), dma((1,)),
            dma((2,)),
        ],
        compiler_params=pltpu.CompilerParams(
            collective_id=0, has_side_effects=True, vmem_limit_bytes=60 * 1024 * 1024
        ),
        cost_estimate=pl.CostEstimate(flops=13 * 10**9, bytes_accessed=10**7, transcendentals=4 * 10**6),
        name="em_step",
    )(embeddings, centroids, log_mix.reshape(8, 128))
    return made.reshape(1024, D).astype(f32), weights.reshape(1024)


def solution(mesh):
    blks, rows = mesh.shape["blk"], mesh.shape["rows"]

    def step(embeddings, centroids, log_mix):
        factor = centroids.shape[0] * blks / (embeddings.shape[0] * blks * rows)
        return local(embeddings, centroids, log_mix, factor)

    return jax.shard_map(
        step,
        mesh=mesh,
        in_specs=(P(("blk", "rows"), None), P("blk", None), P("blk")),
        out_specs=(P("blk", None), P("blk")),
        check_vma=False,
    )
```

```python
import math

import jax
import jax.numpy as jnp
from jax import lax
from jax.experimental import pallas as pl
from jax.experimental.pallas import tpu as pltpu
from jax.sharding import PartitionSpec as P

D = 768
CONCENTRATION = 32.0
LOG2E = 1.4426950408889634
MESH = pl.DeviceIdType.MESH
NT = (((1,), (1,)), ((), ()))
NN = (((1,), (0,)), ((), ()))

ROWS = 512
GROUPS = 4
PIECE = 64


def unit(v):
    v = v.astype(jnp.float32)
    return (v * lax.rsqrt(jnp.sum(v * v, axis=1, keepdims=True) + 1e-6)).astype(jnp.bfloat16)


def kernel(
    factor,
    emb, cen, lm, out, wout,
    xr, cr, xu, cu, lmh, lmc, sc, tr, ps, pb, ma, ra, rc, rs, fh, fr, ob, ms, mr, wo,
    in_sem, a_send, a_recv, d_send, d_recv, b_send, b_recv, t_send, t_recv,
    c_send, c_recv, r_send, r_recv, f_send, f_recv, m_send, m_recv, o_send, o_recv,
    q_send, q_recv, w_send, w_recv, out_sem,
):
    blk, row = lax.axis_index("blk"), lax.axis_index("rows")
    z, hi = blk // 2, blk % 2
    x, lo, c = row // 4, (row // 2) % 2, row % 2
    zp, zm, z2 = (z + 1) % 4, (z + 3) % 4, (z + 2) % 4
    xp, xm, x2 = (x + 1) % 4, (x + 3) % 4, (x + 2) % 4

    def dev(z=z, hi=hi, x=x, lo=lo, c=c):
        return (z * 2 + hi, x * 4 + lo * 2 + c)

    def remote(src, dst, send, recv, to):
        return pltpu.make_async_remote_copy(
            src_ref=src, dst_ref=dst, send_sem=send, recv_sem=recv, device_id=to, device_id_type=MESH
        )

    started = []

    def go(src, dst, send, recv, to):
        copy = remote(src, dst, send, recv, to)
        copy.start()
        started.append(copy)

    def landed(dst, send, recv):
        remote(dst, dst, send, recv, dev(c=1 - c)).wait_recv()

    get_x = pltpu.make_async_copy(emb, xr, in_sem.at[0])
    get_c = pltpu.make_async_copy(cen.at[pl.ds(pl.multiple_of(c * 512, 512), 512)], cr, in_sem.at[1])
    get_x.start()
    get_c.start()

    twin_core = dev(c=1 - c)
    beside = [dev(hi=1 - hi, lo=1 - lo, c=cc) for cc in (0, 1)]

    def end_of(zz):
        return [dev(z=zz, c=cc) for cc in (0, 1)] + [dev(z=zz, hi=1 - hi, lo=1 - lo, c=cc) for cc in (0, 1)]

    line = [twin_core] + beside + end_of(zp) + end_of(zm)
    near = [dev(lo=1 - lo)] + [dev(x=xx, lo=ll) for xx in (xp, xm, x2) for ll in (0, 1)]
    across = [dev(z=z2, x=xx, lo=ll) for xx in range(4) for ll in (0, 1)]
    barrier = pltpu.get_barrier_semaphore()
    for peer in line + near + across:
        pl.semaphore_signal(barrier, inc=1, device_id=peer, device_id_type=MESH)

    get_x.wait()

    def unit_rows(i, _):
        v = unit(xr[pl.ds(pl.multiple_of(i * 64, 64), 64)])
        e = i % 2
        xu[i // 2, ((z + e) % 2) * 2 + e, hi, c] = v
        return 0

    lax.fori_loop(0, ROWS // 64, unit_rows, 0)
    get_c.wait()

    def unit_centroids(i, _):
        cu[i] = unit(cr[pl.ds(pl.multiple_of(i * 64, 64), 64)])
        return 0

    lax.fori_loop(0, 8, unit_centroids, 0)

    def offsets(i, ref, base):
        r = ref[pl.ds(c * 4 + i, 1), :]
        wide = jnp.broadcast_to(r, (128, 128))
        lmc[base + i] = (wide.T - CONCENTRATION) * LOG2E

    for i in range(4):
        offsets(i, lm, 0)

    def clear(i, _):
        ps[i] = jnp.zeros((PIECE, D), jnp.float32)
        return 0

    lax.fori_loop(0, 16, clear, 0)
    ma[...] = jnp.zeros_like(ma)
    pl.semaphore_wait(barrier, len(line + near + across))

    up, down = (z % 2) * 2, ((z + 1) % 2) * 2 + 1
    from_up, from_down = (z % 2) * 2 + 1, ((z + 1) % 2) * 2
    opposite = dev(hi=1 - hi, lo=1 - lo)

    def send_rows(g, slot, h, k, to):
        at = xu.at[g, slot, h, c]
        go(at, at, a_send.at[g, k], a_recv.at[g, k], to)

    def rows_came(g, slot, h, k):
        landed(xu.at[g, slot, h, c], a_send.at[g, k], a_recv.at[g, k])

    def across_out(g):
        send_rows(g, up, hi, 0, opposite)
        send_rows(g, down, hi, 1, opposite)

    def along_out(g):
        send_rows(g, up, hi, 2, dev(z=zp))
        send_rows(g, down, hi, 3, dev(z=zm))

    def share(g, slot, h, k):
        at = xu.at[g, slot, h, c]
        go(at, at, d_send.at[g, k], d_recv.at[g, k], twin_core)

    def relay_rows(g):
        rows_came(g, up, 1 - hi, 0)
        send_rows(g, up, 1 - hi, 4, dev(z=zp))
        rows_came(g, down, 1 - hi, 1)
        send_rows(g, down, 1 - hi, 5, dev(z=zm))
        share(g, up, 1 - hi, 2)
        share(g, down, 1 - hi, 3)

    def near_rows(g):
        rows_came(g, from_down, hi, 2)
        share(g, from_down, hi, 4)
        rows_came(g, from_up, hi, 3)
        share(g, from_up, hi, 5)

    def far_rows(g):
        rows_came(g, from_down, 1 - hi, 4)
        share(g, from_down, 1 - hi, 6)
        rows_came(g, from_up, 1 - hi, 5)
        share(g, from_up, 1 - hi, 7)

    def shared(g):
        for k, (slot, h) in enumerate((
            (up, hi), (down, hi), (up, 1 - hi), (down, 1 - hi),
            (from_down, hi), (from_up, hi), (from_down, 1 - hi), (from_up, 1 - hi),
        )):
            landed(xu.at[g, slot, h, 1 - c], d_send.at[g, k], d_recv.at[g, k])

    def slice_to(xx, ll, k, recv, to):
        at = cu.at[8 + xx * 2 + ll]
        go(at, at, b_send.at[k], b_recv.at[recv], to)

    def slice_came(xx, ll, recv):
        landed(cu.at[8 + xx * 2 + ll], b_send.at[0], b_recv.at[recv])

    across_out(0)
    here = x * 2 + lo
    go(cu.at[here], cu.at[8 + here], b_send.at[7], b_recv.at[7], dev(z=z2))
    go(lm, lmh, b_send.at[8], b_recv.at[8], dev(z=z2))
    along_out(0)
    for g in range(1, GROUPS):
        across_out(g)
    along_out(1)
    for g in range(GROUPS):
        share(g, up, hi, 0)
        share(g, down, hi, 1)

    def slices_out():
        slice_came(x, lo, 7)
        slice_to(x, lo, 4, 0, dev(lo=1 - lo))
        for ll in (0, 1):
            slice_to(x, lo, ll, 1 + lo, dev(x=xp, lo=ll))
            slice_to(x, lo, 2 + ll, 3 + lo, dev(x=xm, lo=ll))

    def slices_on():
        slice_came(xm, 0, 1)
        slice_to(xm, 0, 5, 5, dev(x=xp))
        slice_came(xp, 1, 4)
        slice_to(xp, 1, 6, 6, dev(x=xm))

    def slices_in():
        slice_came(xm, 1, 2)
        slice_came(xp, 0, 3)
        slice_came(x, 1 - lo, 0)
        slice_came(x2, 0, 5)
        slice_came(x2, 1, 6)

    def scores(g, h):
        def add(n, _):
            cos = lax.dot_general(
                cu[pl.ds(h * 8, 8)].reshape(512, D), xu[g, n].reshape(256, D), NT,
                preferred_element_type=jnp.float32,
            )
            off = lmc[pl.ds(h * 4, 4)].reshape(512, 128)
            e = jnp.exp2(cos * (CONCENTRATION * LOG2E) + jnp.concatenate([off] * 2, axis=1))
            sc[g, n, pl.ds(h * 512, 512)] = e
            part = jnp.sum(e, axis=0, keepdims=True)
            side = n // 2
            me = ((z + side) % 2) * 4 + hi * 2 + c
            tr[g, side, me, n % 2] = part if h == 0 else tr[g, side, me, n % 2] + part
            return 0

        lax.fori_loop(0, 4, add, 0, unroll=4)

    def totals_out(g):
        for side, me, ends in ((z % 2, hi * 2 + c, end_of(zp)), ((z + 1) % 2, 4 + hi * 2 + c, end_of(zm))):
            at = tr.at[g, side, me]
            for peer in [twin_core] + beside + ends:
                remote(at, at, t_send.at[g, side], t_recv.at[g, side], peer).start()

    def totals_in(g):
        for side in (0, 1):
            landed(tr.at[g, side, pl.ds(0, 7)], t_send.at[g, side], t_recv.at[g, side])

    def inverse(g):
        return 1.0 / jnp.sum(tr[g], axis=1)

    def weigh(g, begin, end):
        inv = inverse(g)

        def body(i, _):
            acc = ps[pl.ds(i * 4, 4)].reshape(256, D)
            mass = ma[pl.ds(i * 2, 2)].reshape(256, 128)
            resp = []
            for n in range(4):
                r = sc[g, n, pl.ds(pl.multiple_of(i * 256, 256), 256)] * inv[n // 2, n % 2]
                mass = mass + r[:, :128] + r[:, 128:]
                resp.append(r.astype(jnp.bfloat16))
            acc = acc + lax.dot_general(
                jnp.concatenate(resp, axis=1), xu[g].reshape(1024, D), NN, preferred_element_type=jnp.float32
            )
            ps[pl.ds(i * 4, 4)] = acc.reshape(4, PIECE, D)
            ma[pl.ds(i * 2, 2)] = mass.reshape(2, 128, 128)
            return 0

        lax.fori_loop(begin, end, body, 0, unroll=2)

    relay_rows(0)
    along_out(2)
    slices_out()
    near_rows(0)
    relay_rows(1)
    along_out(3)
    slices_on()
    far_rows(0)
    relay_rows(2)
    near_rows(1)
    shared(0)
    scores(0, 0)
    far_rows(1)
    relay_rows(3)
    slices_in()
    near_rows(2)
    landed(lmh, b_send.at[8], b_recv.at[8])
    for i in range(4):
        offsets(i, lmh, 4)
    scores(0, 1)
    totals_out(0)
    shared(1)
    scores(1, 0)
    scores(1, 1)
    totals_out(1)
    far_rows(2)
    near_rows(3)
    totals_in(0)
    weigh(0, 0, 4)
    far_rows(3)
    shared(2)
    scores(2, 0)
    scores(2, 1)
    totals_out(2)
    shared(3)
    scores(3, 0)
    scores(3, 1)
    totals_out(3)
    totals_in(1)
    weigh(1, 0, 4)
    totals_in(2)
    weigh(2, 0, 4)
    totals_in(3)

    def pack(ch):
        def body(i, _):
            pb[i] = ps[i].astype(jnp.bfloat16)
            return 0

        lax.fori_loop(ch * 8, ch * 8 + 8, body, 0)

    def scatter(ch):
        base = ch * 8

        def send(k, src, slot, to):
            go(src, rc.at[ch, slot], c_send.at[ch, k], c_recv.at[ch, slot], to)

        go(pb.at[base + x2 * 2], ra.at[ch, 0], r_send.at[ch, 0], r_recv.at[ch, 0], dev(x=xp))
        go(pb.at[base + x2 * 2 + 1], ra.at[ch, 1], r_send.at[ch, 1], r_recv.at[ch, 1], dev(x=xm))
        send(0, pb.at[base + xp * 2 + 1], lo, dev(x=xp, lo=1))
        send(1, pb.at[base + xm * 2], 2 + lo, dev(x=xm, lo=0))
        send(2, pb.at[base + x * 2 + 1 - lo], 4, dev(lo=1 - lo))

    def relay(ch):
        base = ch * 8
        landed(ra.at[ch, 0], r_send.at[ch, 0], r_recv.at[ch, 0])
        rs[ch, 0] = (ps[base + xp * 2] + ra[ch, 0].astype(jnp.float32)).astype(jnp.bfloat16)
        go(rs.at[ch, 0], rc.at[ch, lo], c_send.at[ch, 3], c_recv.at[ch, lo], dev(x=xp, lo=0))
        landed(ra.at[ch, 1], r_send.at[ch, 1], r_recv.at[ch, 1])
        rs[ch, 1] = (ps[base + xm * 2 + 1] + ra[ch, 1].astype(jnp.float32)).astype(jnp.bfloat16)
        go(rs.at[ch, 1], rc.at[ch, 2 + lo], c_send.at[ch, 4], c_recv.at[ch, 2 + lo], dev(x=xm, lo=1))

    def gathered(ch):
        total = ps[ch * 8 + x * 2 + lo]
        for slot in (4, 0, 1, 2, 3):
            landed(rc.at[ch, slot], c_send.at[ch, 0], c_recv.at[ch, slot])
            total = total + rc[ch, slot].astype(jnp.float32)
        return total

    weigh(3, 2, 4)
    pack(1)
    scatter(1)
    weigh(3, 0, 2)
    pack(0)
    scatter(0)

    for i in range(8):
        r = jnp.sum(ma[i].T, axis=0, keepdims=True)
        ms[i // 4, pl.ds(i % 4, 1)] = r
    mine = x * 2 + lo
    for peer in near:
        remote(ms.at[0], mr.at[mine], m_send, m_recv, peer).start()
    for peer in across:
        remote(ms.at[1], mr.at[8 + mine], m_send, m_recv, peer).start()
    mr[mine] = ms[0]

    relay(1)
    relay(0)
    fh[...] = gathered(1)
    go(fh, fr, f_send.at[0], f_recv.at[0], dev(z=z2))
    total = gathered(0)
    landed(fr, f_send.at[0], f_recv.at[0])
    total = total + fr[...]
    done = total * lax.rsqrt(jnp.sum(total * total, axis=1, keepdims=True) + 1e-6)
    ob[c, x, lo] = done.astype(jnp.bfloat16)

    def hand(xx, ll, k, recv, to):
        at = ob.at[c, xx, ll]
        go(at, at, o_send.at[k], o_recv.at[recv], to)

    def handed(xx, ll, recv):
        landed(ob.at[c, xx, ll], o_send.at[0], o_recv.at[recv])

    def twin(xx, ll, k):
        at = ob.at[c, xx, ll]
        go(at, at, q_send.at[k], q_recv.at[k], dev(c=1 - c))

    for ll in (0, 1):
        hand(x, lo, ll, 1 + lo, dev(x=xp, lo=ll))
        hand(x, lo, 2 + ll, 3 + lo, dev(x=xm, lo=ll))
    hand(x, lo, 4, 0, dev(lo=1 - lo))
    twin(x, lo, 0)

    landed(mr.at[pl.ds(0, 15)], m_send, m_recv)
    wo[c] = jnp.sum(mr[...], axis=0) * factor
    go(wo.at[c], wo.at[c], w_send.at[0], w_recv.at[0], dev(c=1 - c))

    handed(xm, 0, 1)
    hand(xm, 0, 5, 5, dev(x=xp))
    handed(xp, 1, 4)
    hand(xp, 1, 6, 6, dev(x=xm))
    twin(xm, 0, 1)
    twin(xp, 1, 2)
    handed(xm, 1, 2)
    twin(xm, 1, 3)
    handed(xp, 0, 3)
    twin(xp, 0, 4)
    handed(x, 1 - lo, 0)
    twin(x, 1 - lo, 5)
    handed(x2, 0, 5)
    twin(x2, 0, 6)
    handed(x2, 1, 6)
    twin(x2, 1, 7)
    for k, (xx, ll) in enumerate(
        ((x, lo), (xm, 0), (xp, 1), (xm, 1), (xp, 0), (x, 1 - lo), (x2, 0), (x2, 1))
    ):
        landed(ob.at[1 - c, xx, ll], q_send.at[k], q_recv.at[k])
    landed(wo.at[1 - c], w_send.at[0], w_recv.at[0])
    put = pltpu.make_async_copy(ob, out, out_sem.at[0])
    put.start()
    put_w = pltpu.make_async_copy(wo, wout, out_sem.at[1])
    put_w.start()

    for copy in started:
        copy.wait_send()
    everything = dev(c=1 - c)
    for g in range(GROUPS):
        for side in (0, 1):
            all7 = tr.at[g, side, pl.ds(0, 7)]
            remote(all7, all7, t_send.at[g, side], t_recv.at[g, side], everything).wait_send()
    m15 = mr.at[pl.ds(0, 15)]
    remote(m15, m15, m_send, m_recv, everything).wait_send()
    put.wait()
    put_w.wait()


def local(embeddings, centroids, log_mix, factor):
    f32, bf16 = jnp.float32, jnp.bfloat16
    dma = pltpu.SemaphoreType.DMA
    vmem = pltpu.VMEM
    any_spec = pl.BlockSpec(memory_space=pl.ANY)
    body = lambda *refs: kernel(factor, *refs)
    made, weights = pl.pallas_call(
        body,
        out_shape=(
            jax.ShapeDtypeStruct((2, 4, 2, PIECE, D), bf16),
            jax.ShapeDtypeStruct((2, 4, 128), f32),
        ),
        in_specs=[any_spec, any_spec, pl.BlockSpec(memory_space=vmem)],
        out_specs=(any_spec, any_spec),
        scratch_shapes=[
            vmem((ROWS, D), bf16),
            vmem((512, D), bf16),
            vmem((GROUPS, 4, 2, 2, 64, D), bf16),
            vmem((16, PIECE, D), bf16),
            vmem((8, 128), f32),
            vmem((8, 128, 128), f32),
            vmem((4, 4, 1024, 256), f32),
            vmem((GROUPS, 2, 8, 2, 1, 256), f32),
            vmem((16, PIECE, D), f32),
            vmem((16, PIECE, D), bf16),
            vmem((8, 128, 128), f32),
            vmem((2, 2, PIECE, D), bf16),
            vmem((2, 5, PIECE, D), bf16),
            vmem((2, 2, PIECE, D), bf16),
            vmem((PIECE, D), f32),
            vmem((PIECE, D), f32),
            vmem((2, 4, 2, PIECE, D), bf16),
            vmem((2, 4, 128), f32),
            vmem((16, 4, 128), f32),
            vmem((2, 4, 128), f32),
            dma((2,)),
            dma((GROUPS, 6)), dma((GROUPS, 6)),
            dma((GROUPS, 8)), dma((GROUPS, 8)),
            dma((9,)), dma((9,)),
            dma((GROUPS, 2)), dma((GROUPS, 2)),
            dma((2, 5)), dma((2, 5)),
            dma((2, 2)), dma((2, 2)),
            dma((1,)), dma((1,)),
            dma, dma,
            dma((7,)), dma((7,)),
            dma((8,)), dma((8,)),
            dma((1,)), dma((1,)),
            dma((2,)),
        ],
        compiler_params=pltpu.CompilerParams(
            collective_id=0, has_side_effects=True, vmem_limit_bytes=60 * 1024 * 1024
        ),
        cost_estimate=pl.CostEstimate(flops=13 * 10**9, bytes_accessed=10**7, transcendentals=4 * 10**6),
        name="em_step",
    )(embeddings, centroids, log_mix.reshape(8, 128))
    return made.reshape(1024, D).astype(f32), weights.reshape(1024)


def solution(mesh):
    blks, rows = mesh.shape["blk"], mesh.shape["rows"]

    def step(embeddings, centroids, log_mix):
        factor = centroids.shape[0] * blks / (embeddings.shape[0] * blks * rows)
        return local(embeddings, centroids, log_mix, factor)

    return jax.shard_map(
        step,
        mesh=mesh,
        in_specs=(P(("blk", "rows"), None), P("blk", None), P("blk")),
        out_specs=(P("blk", None), P("blk")),
        check_vma=False,
    )
```

```python
import math

import jax
import jax.numpy as jnp
from jax import lax
from jax.experimental import pallas as pl
from jax.experimental.pallas import tpu as pltpu
from jax.sharding import PartitionSpec as P

D = 768
CONCENTRATION = 32.0
LOG2E = 1.4426950408889634
MESH = pl.DeviceIdType.MESH
NT = (((1,), (1,)), ((), ()))
NN = (((1,), (0,)), ((), ()))

ROWS = 512
GROUPS = 4
PIECE = 64


def unit(v):
    v = v.astype(jnp.float32)
    return (v * lax.rsqrt(jnp.sum(v * v, axis=1, keepdims=True) + 1e-6)).astype(jnp.bfloat16)


def kernel(
    factor,
    emb, cen, lm, out, wout,
    xr, cr, xu, cu, lmh, lmc, sc, tr, ps, pb, ma, ra, rc, rs, fh, fr, ob, ms, mr, wo,
    in_sem, a_send, a_recv, d_send, d_recv, b_send, b_recv, t_send, t_recv,
    c_send, c_recv, r_send, r_recv, f_send, f_recv, m_send, m_recv, o_send, o_recv,
    q_send, q_recv, w_send, w_recv, out_sem,
):
    blk, row = lax.axis_index("blk"), lax.axis_index("rows")
    z, hi = blk // 2, blk % 2
    x, lo, c = row // 4, (row // 2) % 2, row % 2
    zp, zm, z2 = (z + 1) % 4, (z + 3) % 4, (z + 2) % 4
    xp, xm, x2 = (x + 1) % 4, (x + 3) % 4, (x + 2) % 4

    def dev(z=z, hi=hi, x=x, lo=lo, c=c):
        return (z * 2 + hi, x * 4 + lo * 2 + c)

    def remote(src, dst, send, recv, to):
        return pltpu.make_async_remote_copy(
            src_ref=src, dst_ref=dst, send_sem=send, recv_sem=recv, device_id=to, device_id_type=MESH
        )

    started = []

    def go(src, dst, send, recv, to):
        copy = remote(src, dst, send, recv, to)
        copy.start()
        started.append(copy)

    def landed(dst, send, recv):
        remote(dst, dst, send, recv, dev(c=1 - c)).wait_recv()

    get_x = pltpu.make_async_copy(emb, xr, in_sem.at[0])
    get_c = pltpu.make_async_copy(cen.at[pl.ds(pl.multiple_of(c * 512, 512), 512)], cr, in_sem.at[1])
    get_x.start()
    get_c.start()

    twin_core = dev(c=1 - c)
    beside = [dev(hi=1 - hi, lo=1 - lo, c=cc) for cc in (0, 1)]

    def end_of(zz):
        return [dev(z=zz, c=cc) for cc in (0, 1)] + [dev(z=zz, hi=1 - hi, lo=1 - lo, c=cc) for cc in (0, 1)]

    line = [twin_core] + beside + end_of(zp) + end_of(zm)
    near = [dev(lo=1 - lo)] + [dev(x=xx, lo=ll) for xx in (xp, xm, x2) for ll in (0, 1)]
    across = [dev(z=z2, x=xx, lo=ll) for xx in range(4) for ll in (0, 1)]
    barrier = pltpu.get_barrier_semaphore()
    greeted = [twin_core, dev(z=zp), dev(z=zm), dev(z=z2), dev(hi=1 - hi, lo=1 - lo)] + near[:5]
    for peer in greeted:
        pl.semaphore_signal(barrier, inc=1, device_id=peer, device_id_type=MESH)

    get_x.wait()

    def unit_rows(i, _):
        v = unit(xr[pl.ds(pl.multiple_of(i * 64, 64), 64)])
        e = i % 2
        xu[i // 2, ((z + e) % 2) * 2 + e, hi, c] = v
        return 0

    lax.fori_loop(0, ROWS // 64, unit_rows, 0)
    get_c.wait()
    here = x * 2 + lo
    cu[here] = unit(cr[pl.ds(pl.multiple_of(here * 64, 64), 64)])

    def offsets(i, ref, base):
        r = ref[pl.ds(c * 4 + i, 1), :]
        wide = jnp.broadcast_to(r, (128, 128))
        lmc[base + i] = (wide.T - CONCENTRATION) * LOG2E

    pl.semaphore_wait(barrier, len(greeted))

    up, down = (z % 2) * 2, ((z + 1) % 2) * 2 + 1
    from_up, from_down = (z % 2) * 2 + 1, ((z + 1) % 2) * 2
    opposite = dev(hi=1 - hi, lo=1 - lo)

    def send_rows(g, slot, h, k, to):
        at = xu.at[g, slot, h, c]
        go(at, at, a_send.at[g, k], a_recv.at[g, k], to)

    def rows_came(g, slot, h, k):
        landed(xu.at[g, slot, h, c], a_send.at[g, k], a_recv.at[g, k])

    def across_out(g):
        send_rows(g, up, hi, 0, opposite)
        send_rows(g, down, hi, 1, opposite)

    def along_out(g):
        send_rows(g, up, hi, 2, dev(z=zp))
        send_rows(g, down, hi, 3, dev(z=zm))

    def share(g, slot, h, k):
        at = xu.at[g, slot, h, c]
        go(at, at, d_send.at[g, k], d_recv.at[g, k], twin_core)

    def relay_rows(g):
        rows_came(g, up, 1 - hi, 0)
        send_rows(g, up, 1 - hi, 4, dev(z=zp))
        rows_came(g, down, 1 - hi, 1)
        send_rows(g, down, 1 - hi, 5, dev(z=zm))
        share(g, up, 1 - hi, 2)
        share(g, down, 1 - hi, 3)

    def near_rows(g):
        rows_came(g, from_down, hi, 2)
        share(g, from_down, hi, 4)
        rows_came(g, from_up, hi, 3)
        share(g, from_up, hi, 5)

    def far_rows(g):
        rows_came(g, from_down, 1 - hi, 4)
        share(g, from_down, 1 - hi, 6)
        rows_came(g, from_up, 1 - hi, 5)
        share(g, from_up, 1 - hi, 7)

    def shared(g):
        for k, (slot, h) in enumerate((
            (up, hi), (down, hi), (up, 1 - hi), (down, 1 - hi),
            (from_down, hi), (from_up, hi), (from_down, 1 - hi), (from_up, 1 - hi),
        )):
            landed(xu.at[g, slot, h, 1 - c], d_send.at[g, k], d_recv.at[g, k])

    def slice_to(xx, ll, k, recv, to):
        at = cu.at[8 + xx * 2 + ll]
        go(at, at, b_send.at[k], b_recv.at[recv], to)

    def slice_came(xx, ll, recv):
        landed(cu.at[8 + xx * 2 + ll], b_send.at[0], b_recv.at[recv])

    across_out(0)
    go(cu.at[here], cu.at[8 + here], b_send.at[7], b_recv.at[7], dev(z=z2))
    go(lm, lmh, b_send.at[8], b_recv.at[8], dev(z=z2))
    along_out(0)
    for g in range(1, GROUPS):
        across_out(g)
    along_out(1)
    for g in range(GROUPS):
        share(g, up, hi, 0)
        share(g, down, hi, 1)

    def slices_out():
        slice_came(x, lo, 7)
        slice_to(x, lo, 4, 0, dev(lo=1 - lo))
        for ll in (0, 1):
            slice_to(x, lo, ll, 1 + lo, dev(x=xp, lo=ll))
            slice_to(x, lo, 2 + ll, 3 + lo, dev(x=xm, lo=ll))

    def slices_on():
        slice_came(xm, 0, 1)
        slice_to(xm, 0, 5, 5, dev(x=xp))
        slice_came(xp, 1, 4)
        slice_to(xp, 1, 6, 6, dev(x=xm))

    def slices_in():
        slice_came(xm, 1, 2)
        slice_came(xp, 0, 3)
        slice_came(x, 1 - lo, 0)
        slice_came(x2, 0, 5)
        slice_came(x2, 1, 6)

    def scores(g, h):
        def add(n, _):
            cos = lax.dot_general(
                cu[pl.ds(h * 8, 8)].reshape(512, D), xu[g, n].reshape(256, D), NT,
                preferred_element_type=jnp.float32,
            )
            off = lmc[pl.ds(h * 4, 4)].reshape(512, 128)
            e = jnp.exp2(cos * (CONCENTRATION * LOG2E) + jnp.concatenate([off] * 2, axis=1))
            sc[g, n, pl.ds(h * 512, 512)] = e
            part = jnp.sum(e, axis=0, keepdims=True)
            side = n // 2
            me = ((z + side) % 2) * 4 + hi * 2 + c
            tr[g, side, me, n % 2] = part if h == 0 else tr[g, side, me, n % 2] + part
            return 0

        lax.fori_loop(0, 4, add, 0, unroll=4)

    def totals_out(g):
        for side, me, ends in ((z % 2, hi * 2 + c, end_of(zp)), ((z + 1) % 2, 4 + hi * 2 + c, end_of(zm))):
            at = tr.at[g, side, me]
            for peer in [twin_core] + beside + ends:
                remote(at, at, t_send.at[g, side], t_recv.at[g, side], peer).start()

    def totals_in(g):
        for side in (0, 1):
            landed(tr.at[g, side, pl.ds(0, 7)], t_send.at[g, side], t_recv.at[g, side])

    def inverse(g):
        return 1.0 / jnp.sum(tr[g], axis=1)

    def weigh(g, begin, end):
        inv = inverse(g)

        def body(i, _):
            acc = ps[pl.ds(i * 4, 4)].reshape(256, D)
            mass = ma[pl.ds(i * 2, 2)].reshape(256, 128)
            resp = []
            for n in range(4):
                r = sc[g, n, pl.ds(pl.multiple_of(i * 256, 256), 256)] * inv[n // 2, n % 2]
                mass = mass + r[:, :128] + r[:, 128:]
                resp.append(r.astype(jnp.bfloat16))
            acc = acc + lax.dot_general(
                jnp.concatenate(resp, axis=1), xu[g].reshape(1024, D), NN, preferred_element_type=jnp.float32
            )
            ps[pl.ds(i * 4, 4)] = acc.reshape(4, PIECE, D)
            ma[pl.ds(i * 2, 2)] = mass.reshape(2, 128, 128)
            return 0

        lax.fori_loop(begin, end, body, 0, unroll=2)

    def unit_centroids(i, _):
        @pl.when(i != here)
        def _():
            cu[i] = unit(cr[pl.ds(pl.multiple_of(i * 64, 64), 64)])

        return 0

    lax.fori_loop(0, 8, unit_centroids, 0)

    for i in range(4):
        offsets(i, lm, 0)

    def clear(i, _):
        ps[i] = jnp.zeros((PIECE, D), jnp.float32)
        return 0

    lax.fori_loop(0, 16, clear, 0)
    ma[...] = jnp.zeros_like(ma)
    relay_rows(0)
    along_out(2)
    slices_out()
    near_rows(0)
    relay_rows(1)
    along_out(3)
    slices_on()
    far_rows(0)
    relay_rows(2)
    near_rows(1)
    shared(0)
    scores(0, 0)
    far_rows(1)
    relay_rows(3)
    near_rows(2)
    near_rows(3)
    far_rows(2)
    slices_in()
    landed(lmh, b_send.at[8], b_recv.at[8])
    for i in range(4):
        offsets(i, lmh, 4)
    scores(0, 1)
    totals_out(0)
    shared(1)
    scores(1, 0)
    scores(1, 1)
    totals_out(1)
    shared(2)
    scores(2, 0)
    scores(2, 1)
    totals_out(2)
    far_rows(3)
    totals_in(0)
    weigh(0, 0, 4)
    shared(3)
    scores(3, 0)
    scores(3, 1)
    totals_out(3)
    totals_in(1)
    weigh(1, 0, 4)
    totals_in(2)
    weigh(2, 0, 4)
    totals_in(3)

    def pack(ch):
        def body(i, _):
            pb[i] = ps[i].astype(jnp.bfloat16)
            return 0

        lax.fori_loop(ch * 8, ch * 8 + 8, body, 0)

    def scatter(ch):
        base = ch * 8

        def send(k, src, slot, to):
            go(src, rc.at[ch, slot], c_send.at[ch, k], c_recv.at[ch, slot], to)

        go(pb.at[base + x2 * 2], ra.at[ch, 0], r_send.at[ch, 0], r_recv.at[ch, 0], dev(x=xp))
        go(pb.at[base + x2 * 2 + 1], ra.at[ch, 1], r_send.at[ch, 1], r_recv.at[ch, 1], dev(x=xm))
        send(0, pb.at[base + xp * 2 + 1], lo, dev(x=xp, lo=1))
        send(1, pb.at[base + xm * 2], 2 + lo, dev(x=xm, lo=0))
        send(2, pb.at[base + x * 2 + 1 - lo], 4, dev(lo=1 - lo))

    def relay(ch):
        base = ch * 8
        landed(ra.at[ch, 0], r_send.at[ch, 0], r_recv.at[ch, 0])
        rs[ch, 0] = (ps[base + xp * 2] + ra[ch, 0].astype(jnp.float32)).astype(jnp.bfloat16)
        go(rs.at[ch, 0], rc.at[ch, lo], c_send.at[ch, 3], c_recv.at[ch, lo], dev(x=xp, lo=0))
        landed(ra.at[ch, 1], r_send.at[ch, 1], r_recv.at[ch, 1])
        rs[ch, 1] = (ps[base + xm * 2 + 1] + ra[ch, 1].astype(jnp.float32)).astype(jnp.bfloat16)
        go(rs.at[ch, 1], rc.at[ch, 2 + lo], c_send.at[ch, 4], c_recv.at[ch, 2 + lo], dev(x=xm, lo=1))

    def gathered(ch):
        total = ps[ch * 8 + x * 2 + lo]
        for slot in (4, 0, 1, 2, 3):
            landed(rc.at[ch, slot], c_send.at[ch, 0], c_recv.at[ch, slot])
            total = total + rc[ch, slot].astype(jnp.float32)
        return total

    weigh(3, 2, 4)
    pack(1)
    scatter(1)
    weigh(3, 0, 2)
    pack(0)
    scatter(0)

    for i in range(8):
        r = jnp.sum(ma[i].T, axis=0, keepdims=True)
        ms[i // 4, pl.ds(i % 4, 1)] = r
    mine = x * 2 + lo
    for peer in near:
        remote(ms.at[0], mr.at[mine], m_send, m_recv, peer).start()
    for peer in across:
        remote(ms.at[1], mr.at[8 + mine], m_send, m_recv, peer).start()
    mr[mine] = ms[0]

    relay(1)
    relay(0)
    fh[...] = gathered(1)
    go(fh, fr, f_send.at[0], f_recv.at[0], dev(z=z2))
    total = gathered(0)
    landed(fr, f_send.at[0], f_recv.at[0])
    total = total + fr[...]
    done = total * lax.rsqrt(jnp.sum(total * total, axis=1, keepdims=True) + 1e-6)
    ob[c, x, lo] = done.astype(jnp.bfloat16)

    def hand(xx, ll, k, recv, to):
        at = ob.at[c, xx, ll]
        go(at, at, o_send.at[k], o_recv.at[recv], to)

    def handed(xx, ll, recv):
        landed(ob.at[c, xx, ll], o_send.at[0], o_recv.at[recv])

    def twin(xx, ll, k):
        at = ob.at[c, xx, ll]
        go(at, at, q_send.at[k], q_recv.at[k], dev(c=1 - c))

    for ll in (0, 1):
        hand(x, lo, ll, 1 + lo, dev(x=xp, lo=ll))
        hand(x, lo, 2 + ll, 3 + lo, dev(x=xm, lo=ll))
    hand(x, lo, 4, 0, dev(lo=1 - lo))
    twin(x, lo, 0)

    landed(mr.at[pl.ds(0, 15)], m_send, m_recv)
    wo[c] = jnp.sum(mr[...], axis=0) * factor
    go(wo.at[c], wo.at[c], w_send.at[0], w_recv.at[0], dev(c=1 - c))

    handed(xm, 0, 1)
    hand(xm, 0, 5, 5, dev(x=xp))
    handed(xp, 1, 4)
    hand(xp, 1, 6, 6, dev(x=xm))
    twin(xm, 0, 1)
    twin(xp, 1, 2)
    handed(xm, 1, 2)
    twin(xm, 1, 3)
    handed(xp, 0, 3)
    twin(xp, 0, 4)
    handed(x, 1 - lo, 0)
    twin(x, 1 - lo, 5)
    pieces = ((x, lo), (xm, 0), (xp, 1), (xm, 1), (xp, 0), (x, 1 - lo), (x2, 0), (x2, 1))
    puts = []

    def put_piece(plane, xx, ll):
        put = pltpu.make_async_copy(ob.at[plane, xx, ll], out.at[plane, xx, ll], out_sem.at[1 + len(puts)])
        put.start()
        puts.append(put)

    for xx, ll in pieces[:6]:
        put_piece(c, xx, ll)
    for k, (xx, ll) in enumerate(pieces[:6]):
        landed(ob.at[1 - c, xx, ll], q_send.at[k], q_recv.at[k])
        put_piece(1 - c, xx, ll)
    for k in (6, 7):
        handed(x2, k - 6, k - 1)
        twin(x2, k - 6, k)
        put_piece(c, x2, k - 6)
    for k in (6, 7):
        landed(ob.at[1 - c, x2, k - 6], q_send.at[k], q_recv.at[k])
        put_piece(1 - c, x2, k - 6)
    landed(wo.at[1 - c], w_send.at[0], w_recv.at[0])
    put_w = pltpu.make_async_copy(wo, wout, out_sem.at[0])
    put_w.start()

    for copy in started:
        copy.wait_send()
    everything = dev(c=1 - c)
    for g in range(GROUPS):
        for side in (0, 1):
            all7 = tr.at[g, side, pl.ds(0, 7)]
            remote(all7, all7, t_send.at[g, side], t_recv.at[g, side], everything).wait_send()
    m15 = mr.at[pl.ds(0, 15)]
    remote(m15, m15, m_send, m_recv, everything).wait_send()
    for put in puts:
        put.wait()
    put_w.wait()


def local(embeddings, centroids, log_mix, factor):
    f32, bf16 = jnp.float32, jnp.bfloat16
    dma = pltpu.SemaphoreType.DMA
    vmem = pltpu.VMEM
    any_spec = pl.BlockSpec(memory_space=pl.ANY)
    body = lambda *refs: kernel(factor, *refs)
    made, weights = pl.pallas_call(
        body,
        out_shape=(
            jax.ShapeDtypeStruct((2, 4, 2, PIECE, D), bf16),
            jax.ShapeDtypeStruct((2, 4, 128), f32),
        ),
        in_specs=[any_spec, any_spec, pl.BlockSpec(memory_space=vmem)],
        out_specs=(any_spec, any_spec),
        scratch_shapes=[
            vmem((ROWS, D), bf16),
            vmem((512, D), bf16),
            vmem((GROUPS, 4, 2, 2, 64, D), bf16),
            vmem((16, PIECE, D), bf16),
            vmem((8, 128), f32),
            vmem((8, 128, 128), f32),
            vmem((4, 4, 1024, 256), f32),
            vmem((GROUPS, 2, 8, 2, 1, 256), f32),
            vmem((16, PIECE, D), f32),
            vmem((16, PIECE, D), bf16),
            vmem((8, 128, 128), f32),
            vmem((2, 2, PIECE, D), bf16),
            vmem((2, 5, PIECE, D), bf16),
            vmem((2, 2, PIECE, D), bf16),
            vmem((PIECE, D), f32),
            vmem((PIECE, D), f32),
            vmem((2, 4, 2, PIECE, D), bf16),
            vmem((2, 4, 128), f32),
            vmem((16, 4, 128), f32),
            vmem((2, 4, 128), f32),
            dma((2,)),
            dma((GROUPS, 6)), dma((GROUPS, 6)),
            dma((GROUPS, 8)), dma((GROUPS, 8)),
            dma((9,)), dma((9,)),
            dma((GROUPS, 2)), dma((GROUPS, 2)),
            dma((2, 5)), dma((2, 5)),
            dma((2, 2)), dma((2, 2)),
            dma((1,)), dma((1,)),
            dma, dma,
            dma((7,)), dma((7,)),
            dma((8,)), dma((8,)),
            dma((1,)), dma((1,)),
            dma((17,)),
        ],
        compiler_params=pltpu.CompilerParams(
            collective_id=0, has_side_effects=True, vmem_limit_bytes=60 * 1024 * 1024
        ),
        cost_estimate=pl.CostEstimate(flops=13 * 10**9, bytes_accessed=10**7, transcendentals=4 * 10**6),
        name="em_step",
    )(embeddings, centroids, log_mix.reshape(8, 128))
    return made.reshape(1024, D).astype(f32), weights.reshape(1024)


def solution(mesh):
    blks, rows = mesh.shape["blk"], mesh.shape["rows"]

    def step(embeddings, centroids, log_mix):
        factor = centroids.shape[0] * blks / (embeddings.shape[0] * blks * rows)
        return local(embeddings, centroids, log_mix, factor)

    return jax.shard_map(
        step,
        mesh=mesh,
        in_specs=(P(("blk", "rows"), None), P("blk", None), P("blk")),
        out_specs=(P("blk", None), P("blk")),
        check_vma=False,
    )
```

```python
import math

import jax
import jax.numpy as jnp
from jax import lax
from jax.experimental import pallas as pl
from jax.experimental.pallas import tpu as pltpu
from jax.sharding import PartitionSpec as P

D = 768
CONCENTRATION = 32.0
LOG2E = 1.4426950408889634
MESH = pl.DeviceIdType.MESH
NT = (((1,), (1,)), ((), ()))
NN = (((1,), (0,)), ((), ()))

ROWS = 512
GROUPS = 4
PIECE = 64


def unit(v):
    v = v.astype(jnp.float32)
    return (v * lax.rsqrt(jnp.sum(v * v, axis=1, keepdims=True) + 1e-6)).astype(jnp.bfloat16)


def kernel(
    factor,
    emb, cen, lm, out, wout,
    xr, cr, xu, cu, lmh, lmc, sc, tr, ps, pb, ma, ra, rc, rs, fh, fr, ob, ms, mr, wo,
    in_sem, a_send, a_recv, d_send, d_recv, b_send, b_recv, t_send, t_recv,
    c_send, c_recv, r_send, r_recv, f_send, f_recv, m_send, m_recv, o_send, o_recv,
    q_send, q_recv, w_send, w_recv, out_sem,
):
    blk, row = lax.axis_index("blk"), lax.axis_index("rows")
    z, hi = blk // 2, blk % 2
    x, lo, c = row // 4, (row // 2) % 2, row % 2
    zp, zm, z2 = (z + 1) % 4, (z + 3) % 4, (z + 2) % 4
    xp, xm, x2 = (x + 1) % 4, (x + 3) % 4, (x + 2) % 4

    def dev(z=z, hi=hi, x=x, lo=lo, c=c):
        return (z * 2 + hi, x * 4 + lo * 2 + c)

    def remote(src, dst, send, recv, to):
        return pltpu.make_async_remote_copy(
            src_ref=src, dst_ref=dst, send_sem=send, recv_sem=recv, device_id=to, device_id_type=MESH
        )

    started = []

    def go(src, dst, send, recv, to):
        copy = remote(src, dst, send, recv, to)
        copy.start()
        started.append(copy)

    def landed(dst, send, recv):
        remote(dst, dst, send, recv, dev(c=1 - c)).wait_recv()

    get_x = pltpu.make_async_copy(emb, xr, in_sem.at[0])
    get_c = pltpu.make_async_copy(cen.at[pl.ds(pl.multiple_of(c * 512, 512), 512)], cr, in_sem.at[1])
    get_x.start()
    get_c.start()

    twin_core = dev(c=1 - c)
    beside = [dev(hi=1 - hi, lo=1 - lo, c=cc) for cc in (0, 1)]

    def end_of(zz):
        return [dev(z=zz, c=cc) for cc in (0, 1)] + [dev(z=zz, hi=1 - hi, lo=1 - lo, c=cc) for cc in (0, 1)]

    line = [twin_core] + beside + end_of(zp) + end_of(zm)
    near = [dev(lo=1 - lo)] + [dev(x=xx, lo=ll) for xx in (xp, xm, x2) for ll in (0, 1)]
    across = [dev(z=z2, x=xx, lo=ll) for xx in range(4) for ll in (0, 1)]
    barrier = pltpu.get_barrier_semaphore()
    greeted = [twin_core, dev(z=zp), dev(z=zm), dev(z=z2), dev(hi=1 - hi, lo=1 - lo)] + near[:5]
    for peer in greeted:
        pl.semaphore_signal(barrier, inc=1, device_id=peer, device_id_type=MESH)

    get_x.wait()

    def unit_rows(i, _):
        v = unit(xr[pl.ds(pl.multiple_of(i * 64, 64), 64)])
        e = i % 2
        xu[i // 2, ((z + e) % 2) * 2 + e, hi, c] = v
        return 0

    lax.fori_loop(0, ROWS // 64, unit_rows, 0)
    get_c.wait()
    here = x * 2 + lo
    cu[here] = unit(cr[pl.ds(pl.multiple_of(here * 64, 64), 64)])

    def offsets(i, ref, base):
        r = ref[pl.ds(c * 4 + i, 1), :]
        wide = jnp.broadcast_to(r, (128, 128))
        lmc[base + i] = (wide.T - CONCENTRATION) * LOG2E

    pl.semaphore_wait(barrier, len(greeted))

    up, down = (z % 2) * 2, ((z + 1) % 2) * 2 + 1
    from_up, from_down = (z % 2) * 2 + 1, ((z + 1) % 2) * 2
    opposite = dev(hi=1 - hi, lo=1 - lo)

    def send_rows(g, slot, h, k, to):
        at = xu.at[g, slot, h, c]
        go(at, at, a_send.at[g, k], a_recv.at[g, k], to)

    def rows_came(g, slot, h, k):
        landed(xu.at[g, slot, h, c], a_send.at[g, k], a_recv.at[g, k])

    def across_out(g):
        send_rows(g, up, hi, 0, opposite)
        send_rows(g, down, hi, 1, opposite)

    def along_out(g):
        send_rows(g, up, hi, 2, dev(z=zp))
        send_rows(g, down, hi, 3, dev(z=zm))

    def share(g, slot, h, k):
        at = xu.at[g, slot, h, c]
        go(at, at, d_send.at[g, k], d_recv.at[g, k], twin_core)

    def relay_rows(g):
        rows_came(g, up, 1 - hi, 0)
        send_rows(g, up, 1 - hi, 4, dev(z=zp))
        rows_came(g, down, 1 - hi, 1)
        send_rows(g, down, 1 - hi, 5, dev(z=zm))
        share(g, up, 1 - hi, 2)
        share(g, down, 1 - hi, 3)

    def near_rows(g):
        rows_came(g, from_down, hi, 2)
        share(g, from_down, hi, 4)
        rows_came(g, from_up, hi, 3)
        share(g, from_up, hi, 5)

    def far_rows(g):
        rows_came(g, from_down, 1 - hi, 4)
        share(g, from_down, 1 - hi, 6)
        rows_came(g, from_up, 1 - hi, 5)
        share(g, from_up, 1 - hi, 7)

    def shared(g):
        for k, (slot, h) in enumerate((
            (up, hi), (down, hi), (up, 1 - hi), (down, 1 - hi),
            (from_down, hi), (from_up, hi), (from_down, 1 - hi), (from_up, 1 - hi),
        )):
            landed(xu.at[g, slot, h, 1 - c], d_send.at[g, k], d_recv.at[g, k])

    def slice_to(xx, ll, k, recv, to):
        at = cu.at[8 + xx * 2 + ll]
        go(at, at, b_send.at[k], b_recv.at[recv], to)

    def slice_came(xx, ll, recv):
        landed(cu.at[8 + xx * 2 + ll], b_send.at[0], b_recv.at[recv])

    across_out(0)
    go(cu.at[here], cu.at[8 + here], b_send.at[7], b_recv.at[7], dev(z=z2))
    go(lm, lmh, b_send.at[8], b_recv.at[8], dev(z=z2))
    along_out(0)
    for g in range(1, GROUPS):
        across_out(g)
    along_out(1)
    for g in range(GROUPS):
        share(g, up, hi, 0)
        share(g, down, hi, 1)

    def slices_out():
        slice_came(x, lo, 7)
        slice_to(x, lo, 4, 0, dev(lo=1 - lo))
        for ll in (0, 1):
            slice_to(x, lo, ll, 1 + lo, dev(x=xp, lo=ll))
            slice_to(x, lo, 2 + ll, 3 + lo, dev(x=xm, lo=ll))

    def slices_on():
        slice_came(xm, 0, 1)
        slice_to(xm, 0, 5, 5, dev(x=xp))
        slice_came(xp, 1, 4)
        slice_to(xp, 1, 6, 6, dev(x=xm))

    def slices_in():
        slice_came(xm, 1, 2)
        slice_came(xp, 0, 3)
        slice_came(x, 1 - lo, 0)
        slice_came(x2, 0, 5)
        slice_came(x2, 1, 6)

    def scores(g, h):
        def add(n, _):
            cos = lax.dot_general(
                cu[pl.ds(h * 8, 8)].reshape(512, D), xu[g, n].reshape(256, D), NT,
                preferred_element_type=jnp.float32,
            )
            off = lmc[pl.ds(h * 4, 4)].reshape(512, 128)
            e = jnp.exp2(cos * (CONCENTRATION * LOG2E) + jnp.concatenate([off] * 2, axis=1))
            sc[g, n, pl.ds(h * 512, 512)] = e
            part = jnp.sum(e, axis=0, keepdims=True)
            side = n // 2
            me = ((z + side) % 2) * 4 + hi * 2 + c
            tr[g, side, me, n % 2] = part if h == 0 else tr[g, side, me, n % 2] + part
            return 0

        lax.fori_loop(0, 4, add, 0, unroll=4)

    def totals_out(g):
        for side, me, ends in ((z % 2, hi * 2 + c, end_of(zp)), ((z + 1) % 2, 4 + hi * 2 + c, end_of(zm))):
            at = tr.at[g, side, me]
            for peer in [twin_core] + beside + ends:
                remote(at, at, t_send.at[g, side], t_recv.at[g, side], peer).start()

    def totals_in(g):
        for side in (0, 1):
            landed(tr.at[g, side, pl.ds(0, 7)], t_send.at[g, side], t_recv.at[g, side])

    def inverse(g):
        return 1.0 / jnp.sum(tr[g], axis=1)

    def weigh(g, begin, end):
        inv = inverse(g)

        def body(i, _):
            acc = ps[pl.ds(i * 4, 4)].reshape(256, D)
            mass = ma[pl.ds(i * 2, 2)].reshape(256, 128)
            resp = []
            for n in range(4):
                r = sc[g, n, pl.ds(pl.multiple_of(i * 256, 256), 256)] * inv[n // 2, n % 2]
                mass = mass + r[:, :128] + r[:, 128:]
                resp.append(r.astype(jnp.bfloat16))
            acc = acc + lax.dot_general(
                jnp.concatenate(resp, axis=1), xu[g].reshape(1024, D), NN, preferred_element_type=jnp.float32
            )
            ps[pl.ds(i * 4, 4)] = acc.reshape(4, PIECE, D)
            ma[pl.ds(i * 2, 2)] = mass.reshape(2, 128, 128)
            return 0

        lax.fori_loop(begin, end, body, 0, unroll=2)

    def unit_centroids(i, _):
        @pl.when(i != here)
        def _():
            cu[i] = unit(cr[pl.ds(pl.multiple_of(i * 64, 64), 64)])

        return 0

    lax.fori_loop(0, 8, unit_centroids, 0)

    for i in range(4):
        offsets(i, lm, 0)

    def clear(i, _):
        ps[i] = jnp.zeros((PIECE, D), jnp.float32)
        return 0

    lax.fori_loop(0, 16, clear, 0)
    ma[...] = jnp.zeros_like(ma)
    relay_rows(0)
    along_out(2)
    slices_out()
    near_rows(0)
    relay_rows(1)
    along_out(3)
    slices_on()
    far_rows(0)
    relay_rows(2)
    near_rows(1)
    shared(0)
    scores(0, 0)
    far_rows(1)
    relay_rows(3)
    near_rows(2)
    near_rows(3)
    far_rows(2)
    slices_in()
    landed(lmh, b_send.at[8], b_recv.at[8])
    for i in range(4):
        offsets(i, lmh, 4)
    scores(0, 1)
    totals_out(0)
    shared(1)
    scores(1, 0)
    scores(1, 1)
    totals_out(1)
    shared(2)
    scores(2, 0)
    scores(2, 1)
    totals_out(2)
    far_rows(3)
    totals_in(0)
    weigh(0, 0, 4)
    shared(3)
    scores(3, 0)
    scores(3, 1)
    totals_out(3)
    totals_in(1)
    weigh(1, 0, 4)
    totals_in(2)
    weigh(2, 0, 4)
    totals_in(3)

    def pack(ch):
        def body(i, _):
            pb[i] = ps[i].astype(jnp.bfloat16)
            return 0

        lax.fori_loop(ch * 8, ch * 8 + 8, body, 0)

    def scatter(ch):
        base = ch * 8
        go(pb.at[base + x2 * 2], ra.at[ch, 0], r_send.at[ch, 0], r_recv.at[ch, 0], dev(x=xp))
        go(pb.at[base + x2 * 2 + 1], ra.at[ch, 1], r_send.at[ch, 1], r_recv.at[ch, 1], dev(x=xm))

    def scatter_direct(ch):
        base = ch * 8

        def send(k, src, slot, to):
            go(src, rc.at[ch, slot], c_send.at[ch, k], c_recv.at[ch, slot], to)

        send(0, pb.at[base + xp * 2 + 1], lo, dev(x=xp, lo=1))
        send(1, pb.at[base + xm * 2], 2 + lo, dev(x=xm, lo=0))
        send(2, pb.at[base + x * 2 + 1 - lo], 4, dev(lo=1 - lo))

    def relay(ch):
        base = ch * 8
        landed(ra.at[ch, 0], r_send.at[ch, 0], r_recv.at[ch, 0])
        rs[ch, 0] = (ps[base + xp * 2] + ra[ch, 0].astype(jnp.float32)).astype(jnp.bfloat16)
        go(rs.at[ch, 0], rc.at[ch, lo], c_send.at[ch, 3], c_recv.at[ch, lo], dev(x=xp, lo=0))
        landed(ra.at[ch, 1], r_send.at[ch, 1], r_recv.at[ch, 1])
        rs[ch, 1] = (ps[base + xm * 2 + 1] + ra[ch, 1].astype(jnp.float32)).astype(jnp.bfloat16)
        go(rs.at[ch, 1], rc.at[ch, 2 + lo], c_send.at[ch, 4], c_recv.at[ch, 2 + lo], dev(x=xm, lo=1))

    def gathered(ch):
        total = ps[ch * 8 + x * 2 + lo]
        for slot in (4, 0, 1, 2, 3):
            landed(rc.at[ch, slot], c_send.at[ch, 0], c_recv.at[ch, slot])
            total = total + rc[ch, slot].astype(jnp.float32)
        return total

    weigh(3, 2, 4)
    pack(1)
    scatter(1)
    scatter_direct(1)
    weigh(3, 0, 2)
    pack(0)
    scatter(0)

    relay(1)
    scatter_direct(0)
    relay(0)
    fh[...] = gathered(1)
    go(fh, fr, f_send.at[0], f_recv.at[0], dev(z=z2))
    for i in range(8):
        r = jnp.sum(ma[i].T, axis=0, keepdims=True)
        ms[i // 4, pl.ds(i % 4, 1)] = r
    mine = x * 2 + lo
    for peer in near:
        remote(ms.at[0], mr.at[mine], m_send, m_recv, peer).start()
    for peer in across:
        remote(ms.at[1], mr.at[8 + mine], m_send, m_recv, peer).start()
    mr[mine] = ms[0]

    total = gathered(0)
    landed(fr, f_send.at[0], f_recv.at[0])
    total = total + fr[...]
    done = total * lax.rsqrt(jnp.sum(total * total, axis=1, keepdims=True) + 1e-6)
    ob[c, x, lo] = done.astype(jnp.bfloat16)

    def hand(xx, ll, k, recv, to):
        at = ob.at[c, xx, ll]
        go(at, at, o_send.at[k], o_recv.at[recv], to)

    def handed(xx, ll, recv):
        landed(ob.at[c, xx, ll], o_send.at[0], o_recv.at[recv])

    def twin(xx, ll, k):
        at = ob.at[c, xx, ll]
        go(at, at, q_send.at[k], q_recv.at[k], dev(c=1 - c))

    for ll in (0, 1):
        hand(x, lo, ll, 1 + lo, dev(x=xp, lo=ll))
        hand(x, lo, 2 + ll, 3 + lo, dev(x=xm, lo=ll))
    hand(x, lo, 4, 0, dev(lo=1 - lo))
    twin(x, lo, 0)

    landed(mr.at[pl.ds(0, 15)], m_send, m_recv)
    wo[c] = jnp.sum(mr[...], axis=0) * factor
    go(wo.at[c], wo.at[c], w_send.at[0], w_recv.at[0], dev(c=1 - c))

    handed(xm, 0, 1)
    hand(xm, 0, 5, 5, dev(x=xp))
    handed(xp, 1, 4)
    hand(xp, 1, 6, 6, dev(x=xm))
    twin(xm, 0, 1)
    twin(xp, 1, 2)
    handed(xm, 1, 2)
    twin(xm, 1, 3)
    handed(xp, 0, 3)
    twin(xp, 0, 4)
    handed(x, 1 - lo, 0)
    twin(x, 1 - lo, 5)
    pieces = ((x, lo), (xm, 0), (xp, 1), (xm, 1), (xp, 0), (x, 1 - lo), (x2, 0), (x2, 1))
    puts = []

    def put_piece(plane, xx, ll):
        put = pltpu.make_async_copy(ob.at[plane, xx, ll], out.at[plane, xx, ll], out_sem.at[1 + len(puts)])
        put.start()
        puts.append(put)

    for xx, ll in pieces[:6]:
        put_piece(c, xx, ll)
    for k, (xx, ll) in enumerate(pieces[:6]):
        landed(ob.at[1 - c, xx, ll], q_send.at[k], q_recv.at[k])
        put_piece(1 - c, xx, ll)
    for k in (6, 7):
        handed(x2, k - 6, k - 1)
        twin(x2, k - 6, k)
        put_piece(c, x2, k - 6)
    for k in (6, 7):
        landed(ob.at[1 - c, x2, k - 6], q_send.at[k], q_recv.at[k])
        put_piece(1 - c, x2, k - 6)
    landed(wo.at[1 - c], w_send.at[0], w_recv.at[0])
    put_w = pltpu.make_async_copy(wo, wout, out_sem.at[0])
    put_w.start()

    for copy in started:
        copy.wait_send()
    everything = dev(c=1 - c)
    for g in range(GROUPS):
        for side in (0, 1):
            all7 = tr.at[g, side, pl.ds(0, 7)]
            remote(all7, all7, t_send.at[g, side], t_recv.at[g, side], everything).wait_send()
    m15 = mr.at[pl.ds(0, 15)]
    remote(m15, m15, m_send, m_recv, everything).wait_send()
    for put in puts:
        put.wait()
    put_w.wait()


def local(embeddings, centroids, log_mix, factor):
    f32, bf16 = jnp.float32, jnp.bfloat16
    dma = pltpu.SemaphoreType.DMA
    vmem = pltpu.VMEM
    any_spec = pl.BlockSpec(memory_space=pl.ANY)
    body = lambda *refs: kernel(factor, *refs)
    made, weights = pl.pallas_call(
        body,
        out_shape=(
            jax.ShapeDtypeStruct((2, 4, 2, PIECE, D), bf16),
            jax.ShapeDtypeStruct((2, 4, 128), f32),
        ),
        in_specs=[any_spec, any_spec, pl.BlockSpec(memory_space=vmem)],
        out_specs=(any_spec, any_spec),
        scratch_shapes=[
            vmem((ROWS, D), bf16),
            vmem((512, D), bf16),
            vmem((GROUPS, 4, 2, 2, 64, D), bf16),
            vmem((16, PIECE, D), bf16),
            vmem((8, 128), f32),
            vmem((8, 128, 128), f32),
            vmem((4, 4, 1024, 256), f32),
            vmem((GROUPS, 2, 8, 2, 1, 256), f32),
            vmem((16, PIECE, D), f32),
            vmem((16, PIECE, D), bf16),
            vmem((8, 128, 128), f32),
            vmem((2, 2, PIECE, D), bf16),
            vmem((2, 5, PIECE, D), bf16),
            vmem((2, 2, PIECE, D), bf16),
            vmem((PIECE, D), f32),
            vmem((PIECE, D), f32),
            vmem((2, 4, 2, PIECE, D), bf16),
            vmem((2, 4, 128), f32),
            vmem((16, 4, 128), f32),
            vmem((2, 4, 128), f32),
            dma((2,)),
            dma((GROUPS, 6)), dma((GROUPS, 6)),
            dma((GROUPS, 8)), dma((GROUPS, 8)),
            dma((9,)), dma((9,)),
            dma((GROUPS, 2)), dma((GROUPS, 2)),
            dma((2, 5)), dma((2, 5)),
            dma((2, 2)), dma((2, 2)),
            dma((1,)), dma((1,)),
            dma, dma,
            dma((7,)), dma((7,)),
            dma((8,)), dma((8,)),
            dma((1,)), dma((1,)),
            dma((17,)),
        ],
        compiler_params=pltpu.CompilerParams(
            collective_id=0, has_side_effects=True, vmem_limit_bytes=60 * 1024 * 1024
        ),
        cost_estimate=pl.CostEstimate(flops=13 * 10**9, bytes_accessed=10**7, transcendentals=4 * 10**6),
        name="em_step",
    )(embeddings, centroids, log_mix.reshape(8, 128))
    return made.reshape(1024, D).astype(f32), weights.reshape(1024)


def solution(mesh):
    blks, rows = mesh.shape["blk"], mesh.shape["rows"]

    def step(embeddings, centroids, log_mix):
        factor = centroids.shape[0] * blks / (embeddings.shape[0] * blks * rows)
        return local(embeddings, centroids, log_mix, factor)

    return jax.shard_map(
        step,
        mesh=mesh,
        in_specs=(P(("blk", "rows"), None), P("blk", None), P("blk")),
        out_specs=(P("blk", None), P("blk")),
        check_vma=False,
    )
```

```python
import math

import jax
import jax.numpy as jnp
from jax import lax
from jax.experimental import pallas as pl
from jax.experimental.pallas import tpu as pltpu
from jax.sharding import PartitionSpec as P

D = 768
CONCENTRATION = 32.0
LOG2E = 1.4426950408889634
MESH = pl.DeviceIdType.MESH
NT = (((1,), (1,)), ((), ()))
NN = (((1,), (0,)), ((), ()))

ROWS = 512
GROUPS = 4
PIECE = 64


def unit(v):
    v = v.astype(jnp.float32)
    return (v * lax.rsqrt(jnp.sum(v * v, axis=1, keepdims=True) + 1e-6)).astype(jnp.bfloat16)


def kernel(
    factor,
    emb, cen, lm, out, wout,
    xr, cr, xu, cu, lmh, lmc, sc, tr, ps, pb, ma, ra, rc, rs, fh, fr, ob, ms, mr, wo,
    in_sem, a_send, a_recv, d_send, d_recv, b_send, b_recv, t_send, t_recv,
    c_send, c_recv, r_send, r_recv, f_send, f_recv, m_send, m_recv, o_send, o_recv,
    q_send, q_recv, w_send, w_recv, out_sem,
):
    blk, row = lax.axis_index("blk"), lax.axis_index("rows")
    z, hi = blk // 2, blk % 2
    x, lo, c = row // 4, (row // 2) % 2, row % 2
    zp, zm, z2 = (z + 1) % 4, (z + 3) % 4, (z + 2) % 4
    xp, xm, x2 = (x + 1) % 4, (x + 3) % 4, (x + 2) % 4

    def dev(z=z, hi=hi, x=x, lo=lo, c=c):
        return (z * 2 + hi, x * 4 + lo * 2 + c)

    def remote(src, dst, send, recv, to):
        return pltpu.make_async_remote_copy(
            src_ref=src, dst_ref=dst, send_sem=send, recv_sem=recv, device_id=to, device_id_type=MESH
        )

    started = []

    def go(src, dst, send, recv, to):
        copy = remote(src, dst, send, recv, to)
        copy.start()
        started.append(copy)

    def landed(dst, send, recv):
        remote(dst, dst, send, recv, dev(c=1 - c)).wait_recv()

    get_x = pltpu.make_async_copy(emb, xr, in_sem.at[0])
    get_c = pltpu.make_async_copy(cen.at[pl.ds(pl.multiple_of(c * 512, 512), 512)], cr, in_sem.at[1])
    get_x.start()
    get_c.start()

    twin_core = dev(c=1 - c)
    beside = [dev(hi=1 - hi, lo=1 - lo, c=cc) for cc in (0, 1)]

    def end_of(zz):
        return [dev(z=zz, c=cc) for cc in (0, 1)] + [dev(z=zz, hi=1 - hi, lo=1 - lo, c=cc) for cc in (0, 1)]

    line = [twin_core] + beside + end_of(zp) + end_of(zm)
    near = [dev(lo=1 - lo)] + [dev(x=xx, lo=ll) for xx in (xp, xm, x2) for ll in (0, 1)]
    across = [dev(z=z2, x=xx, lo=ll) for xx in range(4) for ll in (0, 1)]
    barrier = pltpu.get_barrier_semaphore()
    greeted = [twin_core, dev(z=zp), dev(z=zm), dev(z=z2), dev(hi=1 - hi, lo=1 - lo)] + near[:5]
    for peer in greeted:
        pl.semaphore_signal(barrier, inc=1, device_id=peer, device_id_type=MESH)

    get_x.wait()

    def unit_rows(i, _):
        v = unit(xr[pl.ds(pl.multiple_of(i * 64, 64), 64)])
        e = i % 2
        xu[i // 2, ((z + e) % 2) * 2 + e, hi, c] = v
        return 0

    lax.fori_loop(0, ROWS // 64, unit_rows, 0)
    get_c.wait()
    here = x * 2 + lo
    cu[here] = unit(cr[pl.ds(pl.multiple_of(here * 64, 64), 64)])

    def offsets(i, ref, base):
        r = ref[pl.ds(c * 4 + i, 1), :]
        wide = jnp.broadcast_to(r, (128, 128))
        lmc[base + i] = (wide.T - CONCENTRATION) * LOG2E

    pl.semaphore_wait(barrier, len(greeted))

    up, down = (z % 2) * 2, ((z + 1) % 2) * 2 + 1
    from_up, from_down = (z % 2) * 2 + 1, ((z + 1) % 2) * 2
    opposite = dev(hi=1 - hi, lo=1 - lo)

    def send_rows(g, slot, h, k, to):
        at = xu.at[g, slot, h, c]
        go(at, at, a_send.at[g, k], a_recv.at[g, k], to)

    def rows_came(g, slot, h, k):
        landed(xu.at[g, slot, h, c], a_send.at[g, k], a_recv.at[g, k])

    def across_out(g):
        send_rows(g, up, hi, 0, opposite)
        send_rows(g, down, hi, 1, opposite)

    def along_out(g):
        send_rows(g, up, hi, 2, dev(z=zp))
        send_rows(g, down, hi, 3, dev(z=zm))

    def share(g, slot, h, k):
        at = xu.at[g, slot, h, c]
        go(at, at, d_send.at[g, k], d_recv.at[g, k], twin_core)

    def relay_rows(g):
        rows_came(g, up, 1 - hi, 0)
        send_rows(g, up, 1 - hi, 4, dev(z=zp))
        rows_came(g, down, 1 - hi, 1)
        send_rows(g, down, 1 - hi, 5, dev(z=zm))
        share(g, up, 1 - hi, 2)
        share(g, down, 1 - hi, 3)

    def near_rows(g):
        rows_came(g, from_down, hi, 2)
        share(g, from_down, hi, 4)
        rows_came(g, from_up, hi, 3)
        share(g, from_up, hi, 5)

    def far_rows(g):
        rows_came(g, from_down, 1 - hi, 4)
        share(g, from_down, 1 - hi, 6)
        rows_came(g, from_up, 1 - hi, 5)
        share(g, from_up, 1 - hi, 7)

    def shared(g):
        for k, (slot, h) in enumerate((
            (up, hi), (down, hi), (up, 1 - hi), (down, 1 - hi),
            (from_down, hi), (from_up, hi), (from_down, 1 - hi), (from_up, 1 - hi),
        )):
            landed(xu.at[g, slot, h, 1 - c], d_send.at[g, k], d_recv.at[g, k])

    def slice_to(xx, ll, k, recv, to):
        at = cu.at[8 + xx * 2 + ll]
        go(at, at, b_send.at[k], b_recv.at[recv], to)

    def slice_came(xx, ll, recv):
        landed(cu.at[8 + xx * 2 + ll], b_send.at[0], b_recv.at[recv])

    across_out(0)
    go(cu.at[here], cu.at[8 + here], b_send.at[7], b_recv.at[7], dev(z=z2))
    go(lm, lmh, b_send.at[8], b_recv.at[8], dev(z=z2))
    along_out(0)
    for g in range(1, GROUPS):
        across_out(g)
    along_out(1)
    for g in range(GROUPS):
        share(g, up, hi, 0)
        share(g, down, hi, 1)

    def slices_out():
        slice_came(x, lo, 7)
        slice_to(x, lo, 4, 0, dev(lo=1 - lo))
        for ll in (0, 1):
            slice_to(x, lo, ll, 1 + lo, dev(x=xp, lo=ll))
            slice_to(x, lo, 2 + ll, 3 + lo, dev(x=xm, lo=ll))

    def slices_on():
        slice_came(xm, 0, 1)
        slice_to(xm, 0, 5, 5, dev(x=xp))
        slice_came(xp, 1, 4)
        slice_to(xp, 1, 6, 6, dev(x=xm))

    def slices_in():
        slice_came(xm, 1, 2)
        slice_came(xp, 0, 3)
        slice_came(x, 1 - lo, 0)
        slice_came(x2, 0, 5)
        slice_came(x2, 1, 6)

    def scores(g, h):
        def add(n, _):
            cos = lax.dot_general(
                cu[pl.ds(h * 8, 8)].reshape(512, D), xu[g, n].reshape(256, D), NT,
                preferred_element_type=jnp.float32,
            )
            off = lmc[pl.ds(h * 4, 4)].reshape(512, 128)
            e = jnp.exp2(cos * (CONCENTRATION * LOG2E) + jnp.concatenate([off] * 2, axis=1))
            sc[g, n, pl.ds(h * 512, 512)] = e
            part = jnp.sum(e, axis=0, keepdims=True)
            side = n // 2
            me = ((z + side) % 2) * 4 + hi * 2 + c
            tr[g, side, me, n % 2] = part if h == 0 else tr[g, side, me, n % 2] + part
            return 0

        lax.fori_loop(0, 4, add, 0, unroll=4)

    def totals_out(g):
        for side, me, ends in ((z % 2, hi * 2 + c, end_of(zp)), ((z + 1) % 2, 4 + hi * 2 + c, end_of(zm))):
            at = tr.at[g, side, me]
            for peer in [twin_core] + beside + ends:
                remote(at, at, t_send.at[g, side], t_recv.at[g, side], peer).start()

    def totals_in(g):
        for side in (0, 1):
            landed(tr.at[g, side, pl.ds(0, 7)], t_send.at[g, side], t_recv.at[g, side])

    def inverse(g):
        return 1.0 / jnp.sum(tr[g], axis=1)

    def weigh(g, begin, end):
        inv = inverse(g)

        def body(i, _):
            acc = ps[pl.ds(i * 4, 4)].reshape(256, D)
            mass = ma[pl.ds(i * 2, 2)].reshape(256, 128)
            resp = []
            for n in range(4):
                r = sc[g, n, pl.ds(pl.multiple_of(i * 256, 256), 256)] * inv[n // 2, n % 2]
                mass = mass + r[:, :128] + r[:, 128:]
                resp.append(r.astype(jnp.bfloat16))
            acc = acc + lax.dot_general(
                jnp.concatenate(resp, axis=1), xu[g].reshape(1024, D), NN, preferred_element_type=jnp.float32
            )
            ps[pl.ds(i * 4, 4)] = acc.reshape(4, PIECE, D)
            ma[pl.ds(i * 2, 2)] = mass.reshape(2, 128, 128)
            return 0

        lax.fori_loop(begin, end, body, 0, unroll=2)

    def unit_centroids(i, _):
        @pl.when(i != here)
        def _():
            cu[i] = unit(cr[pl.ds(pl.multiple_of(i * 64, 64), 64)])

        return 0

    lax.fori_loop(0, 8, unit_centroids, 0)

    for i in range(4):
        offsets(i, lm, 0)

    def clear(i, _):
        ps[i] = jnp.zeros((PIECE, D), jnp.float32)
        return 0

    lax.fori_loop(0, 16, clear, 0)
    ma[...] = jnp.zeros_like(ma)
    relay_rows(0)
    along_out(2)
    slices_out()
    near_rows(0)
    relay_rows(1)
    along_out(3)
    slices_on()
    far_rows(0)
    relay_rows(2)
    near_rows(1)
    shared(0)
    scores(0, 0)
    far_rows(1)
    relay_rows(3)
    near_rows(2)
    near_rows(3)
    far_rows(2)
    slices_in()
    landed(lmh, b_send.at[8], b_recv.at[8])
    for i in range(4):
        offsets(i, lmh, 4)
    scores(0, 1)
    totals_out(0)
    shared(1)
    scores(1, 0)
    scores(1, 1)
    totals_out(1)
    shared(2)
    scores(2, 0)
    scores(2, 1)
    totals_out(2)
    far_rows(3)
    totals_in(0)
    weigh(0, 0, 4)
    shared(3)
    scores(3, 0)
    scores(3, 1)
    totals_out(3)
    totals_in(1)
    weigh(1, 0, 4)
    totals_in(2)
    weigh(2, 0, 4)
    totals_in(3)

    def pack(ch):
        def body(i, _):
            pb[i] = ps[i].astype(jnp.bfloat16)
            return 0

        lax.fori_loop(ch * 8, ch * 8 + 8, body, 0)

    def scatter(ch):
        base = ch * 8
        go(pb.at[base + x2 * 2], ra.at[ch, 0], r_send.at[ch, 0], r_recv.at[ch, 0], dev(x=xp))
        go(pb.at[base + x2 * 2 + 1], ra.at[ch, 1], r_send.at[ch, 1], r_recv.at[ch, 1], dev(x=xm))

    def scatter_direct(ch):
        base = ch * 8

        def send(k, src, slot, to):
            go(src, rc.at[ch, slot], c_send.at[ch, k], c_recv.at[ch, slot], to)

        send(0, pb.at[base + xp * 2 + 1], lo, dev(x=xp, lo=1))
        send(1, pb.at[base + xm * 2], 2 + lo, dev(x=xm, lo=0))
        send(2, pb.at[base + x * 2 + 1 - lo], 4, dev(lo=1 - lo))

    def relay(ch):
        base = ch * 8
        landed(ra.at[ch, 0], r_send.at[ch, 0], r_recv.at[ch, 0])
        rs[ch, 0] = (ps[base + xp * 2] + ra[ch, 0].astype(jnp.float32)).astype(jnp.bfloat16)
        go(rs.at[ch, 0], rc.at[ch, lo], c_send.at[ch, 3], c_recv.at[ch, lo], dev(x=xp, lo=0))
        landed(ra.at[ch, 1], r_send.at[ch, 1], r_recv.at[ch, 1])
        rs[ch, 1] = (ps[base + xm * 2 + 1] + ra[ch, 1].astype(jnp.float32)).astype(jnp.bfloat16)
        go(rs.at[ch, 1], rc.at[ch, 2 + lo], c_send.at[ch, 4], c_recv.at[ch, 2 + lo], dev(x=xm, lo=1))

    def gathered(ch):
        total = ps[ch * 8 + x * 2 + lo]
        for slot in (4, 0, 1, 2, 3):
            landed(rc.at[ch, slot], c_send.at[ch, 0], c_recv.at[ch, slot])
            total = total + rc[ch, slot].astype(jnp.float32)
        return total

    weigh(3, 2, 4)
    pack(1)
    scatter(1)
    scatter_direct(1)
    weigh(3, 0, 2)
    pack(0)
    scatter(0)

    relay(1)
    scatter_direct(0)
    relay(0)
    fh[...] = gathered(1)
    go(fh, fr, f_send.at[0], f_recv.at[0], dev(z=z2))
    for i in range(8):
        r = jnp.sum(ma[i].T, axis=0, keepdims=True)
        ms[i // 4, pl.ds(i % 4, 1)] = r
    mine = x * 2 + lo
    for peer in near:
        remote(ms.at[0], mr.at[mine], m_send, m_recv, peer).start()
    for peer in across:
        remote(ms.at[1], mr.at[8 + mine], m_send, m_recv, peer).start()
    mr[mine] = ms[0]

    total = gathered(0)
    landed(fr, f_send.at[0], f_recv.at[0])
    total = total + fr[...]
    done = total * lax.rsqrt(jnp.sum(total * total, axis=1, keepdims=True) + 1e-6)
    ob[c, x, lo] = done.astype(jnp.bfloat16)

    def hand(xx, ll, k, recv, to):
        at = ob.at[c, xx, ll]
        go(at, at, o_send.at[k], o_recv.at[recv], to)

    def handed(xx, ll, recv):
        landed(ob.at[c, xx, ll], o_send.at[0], o_recv.at[recv])

    def twin(xx, ll, k):
        at = ob.at[c, xx, ll]
        go(at, at, q_send.at[k], q_recv.at[k], dev(c=1 - c))

    for ll in (0, 1):
        hand(x, lo, ll, 1 + lo, dev(x=xp, lo=ll))
        hand(x, lo, 2 + ll, 3 + lo, dev(x=xm, lo=ll))
    hand(x, lo, 4, 0, dev(lo=1 - lo))
    twin(x, lo, 0)

    handed(xm, 0, 1)
    hand(xm, 0, 5, 5, dev(x=xp))
    handed(xp, 1, 4)
    hand(xp, 1, 6, 6, dev(x=xm))
    twin(xm, 0, 1)
    twin(xp, 1, 2)
    handed(xm, 1, 2)
    twin(xm, 1, 3)
    handed(xp, 0, 3)
    twin(xp, 0, 4)
    handed(x, 1 - lo, 0)
    twin(x, 1 - lo, 5)

    landed(mr.at[pl.ds(0, 15)], m_send, m_recv)
    wo[c] = jnp.sum(mr[...], axis=0) * factor
    go(wo.at[c], wo.at[c], w_send.at[0], w_recv.at[0], dev(c=1 - c))
    pieces = ((x, lo), (xm, 0), (xp, 1), (xm, 1), (xp, 0), (x, 1 - lo), (x2, 0), (x2, 1))
    puts = []

    def put_piece(plane, xx, ll):
        put = pltpu.make_async_copy(ob.at[plane, xx, ll], out.at[plane, xx, ll], out_sem.at[1 + len(puts)])
        put.start()
        puts.append(put)

    for xx, ll in pieces[:6]:
        put_piece(c, xx, ll)
    for k, (xx, ll) in enumerate(pieces[:6]):
        landed(ob.at[1 - c, xx, ll], q_send.at[k], q_recv.at[k])
        put_piece(1 - c, xx, ll)
    for k in (6, 7):
        handed(x2, k - 6, k - 1)
        twin(x2, k - 6, k)
        put_piece(c, x2, k - 6)
    for k in (6, 7):
        landed(ob.at[1 - c, x2, k - 6], q_send.at[k], q_recv.at[k])
        put_piece(1 - c, x2, k - 6)
    landed(wo.at[1 - c], w_send.at[0], w_recv.at[0])
    put_w = pltpu.make_async_copy(wo, wout, out_sem.at[0])
    put_w.start()

    for copy in started:
        copy.wait_send()
    everything = dev(c=1 - c)
    for g in range(GROUPS):
        for side in (0, 1):
            all7 = tr.at[g, side, pl.ds(0, 7)]
            remote(all7, all7, t_send.at[g, side], t_recv.at[g, side], everything).wait_send()
    m15 = mr.at[pl.ds(0, 15)]
    remote(m15, m15, m_send, m_recv, everything).wait_send()
    for put in puts:
        put.wait()
    put_w.wait()


def local(embeddings, centroids, log_mix, factor):
    f32, bf16 = jnp.float32, jnp.bfloat16
    dma = pltpu.SemaphoreType.DMA
    vmem = pltpu.VMEM
    any_spec = pl.BlockSpec(memory_space=pl.ANY)
    body = lambda *refs: kernel(factor, *refs)
    made, weights = pl.pallas_call(
        body,
        out_shape=(
            jax.ShapeDtypeStruct((2, 4, 2, PIECE, D), bf16),
            jax.ShapeDtypeStruct((2, 4, 128), f32),
        ),
        in_specs=[any_spec, any_spec, pl.BlockSpec(memory_space=vmem)],
        out_specs=(any_spec, any_spec),
        scratch_shapes=[
            vmem((ROWS, D), bf16),
            vmem((512, D), bf16),
            vmem((GROUPS, 4, 2, 2, 64, D), bf16),
            vmem((16, PIECE, D), bf16),
            vmem((8, 128), f32),
            vmem((8, 128, 128), f32),
            vmem((4, 4, 1024, 256), f32),
            vmem((GROUPS, 2, 8, 2, 1, 256), f32),
            vmem((16, PIECE, D), f32),
            vmem((16, PIECE, D), bf16),
            vmem((8, 128, 128), f32),
            vmem((2, 2, PIECE, D), bf16),
            vmem((2, 5, PIECE, D), bf16),
            vmem((2, 2, PIECE, D), bf16),
            vmem((PIECE, D), f32),
            vmem((PIECE, D), f32),
            vmem((2, 4, 2, PIECE, D), bf16),
            vmem((2, 4, 128), f32),
            vmem((16, 4, 128), f32),
            vmem((2, 4, 128), f32),
            dma((2,)),
            dma((GROUPS, 6)), dma((GROUPS, 6)),
            dma((GROUPS, 8)), dma((GROUPS, 8)),
            dma((9,)), dma((9,)),
            dma((GROUPS, 2)), dma((GROUPS, 2)),
            dma((2, 5)), dma((2, 5)),
            dma((2, 2)), dma((2, 2)),
            dma((1,)), dma((1,)),
            dma, dma,
            dma((7,)), dma((7,)),
            dma((8,)), dma((8,)),
            dma((1,)), dma((1,)),
            dma((17,)),
        ],
        compiler_params=pltpu.CompilerParams(
            collective_id=0, has_side_effects=True, vmem_limit_bytes=60 * 1024 * 1024
        ),
        cost_estimate=pl.CostEstimate(flops=13 * 10**9, bytes_accessed=10**7, transcendentals=4 * 10**6),
        name="em_step",
    )(embeddings, centroids, log_mix.reshape(8, 128))
    return made.reshape(1024, D).astype(f32), weights.reshape(1024)


def solution(mesh):
    blks, rows = mesh.shape["blk"], mesh.shape["rows"]

    def step(embeddings, centroids, log_mix):
        factor = centroids.shape[0] * blks / (embeddings.shape[0] * blks * rows)
        return local(embeddings, centroids, log_mix, factor)

    return jax.shard_map(
        step,
        mesh=mesh,
        in_specs=(P(("blk", "rows"), None), P("blk", None), P("blk")),
        out_specs=(P("blk", None), P("blk")),
        check_vma=False,
    )
```
